256 devices in a mesh: rep: 1, dp: 256 (over x, y, z, core).
Axes of the slice: x: 4, y: 4, z: 8, core: 2. Of those that a mesh axis runs over, the one named last changes fastest.
Arguments:
- x: bfloat16 [256, 1024, 768], P(('rep', 'dp'))
- dy: bfloat16 [256, 1024, 768], P(('rep', 'dp'))
- wq: bfloat16 [1, 768, 768], replicated
- wk: bfloat16 [1, 768, 256], replicated
- wv: bfloat16 [1, 768, 256], replicated
- wo: bfloat16 [1, 768, 768], replicated
- w_gate: bfloat16 [1, 768, 2304], replicated
- w_up: bfloat16 [1, 768, 2304], replicated
- w_down: bfloat16 [1, 2304, 768], replicated
- m_wq: float32 [1, 768, 768], replicated
- m_wk: float32 [1, 768, 256], replicated
- m_wv: float32 [1, 768, 256], replicated
- m_wo: float32 [1, 768, 768], replicated
- m_w_gate: float32 [1, 768, 2304], replicated
- m_w_up: float32 [1, 768, 2304], replicated
- m_w_down: float32 [1, 2304, 768], replicated
- v_wq: float32 [1, 768, 768], replicated
- v_wk: float32 [1, 768, 256], replicated
- v_wv: float32 [1, 768, 256], replicated
- v_wo: float32 [1, 768, 768], replicated
- v_w_gate: float32 [1, 768, 2304], replicated
- v_w_up: float32 [1, 768, 2304], replicated
- v_w_down: float32 [1, 2304, 768], replicated
Outputs:
- output 1: bfloat16 [1, 768, 768], P('rep')
- output 2: bfloat16 [1, 768, 256], P('rep')
- output 3: bfloat16 [1, 768, 256], P('rep')
- output 4: bfloat16 [1, 768, 768], P('rep')
- output 5: bfloat16 [1, 768, 2304], P('rep')
- output 6: bfloat16 [1, 768, 2304], P('rep')
- output 7: bfloat16 [1, 2304, 768], P('rep')
- output 8: float32 [1, 768, 768], P('rep')
- output 9: float32 [1, 768, 256], P('rep')
- output 10: float32 [1, 768, 256], P('rep')
- output 11: float32 [1, 768, 768], P('rep')
- output 12: float32 [1, 768, 2304], P('rep')
- output 13: float32 [1, 768, 2304], P('rep')
- output 14: float32 [1, 2304, 768], P('rep')
- output 15: float32 [1, 768, 768], P('rep')
- output 16: float32 [1, 768, 256], P('rep')
- output 17: float32 [1, 768, 256], P('rep')
- output 18: float32 [1, 768, 768], P('rep')
- output 19: float32 [1, 768, 2304], P('rep')
- output 20: float32 [1, 768, 2304], P('rep')
- output 21: float32 [1, 2304, 768], P('rep')
All inputs are finite; a program needn't handle non-finite values.
Results may differ from the reference program's by a relative error of at most 0.024.
Values are sent between devices in bfloat16 or wider.
A program may use at most 768 MiB of HBM per device.

```python
import jax
import jax.numpy as jnp
from jax import lax

SEQUENCES = 256
TOKENS = 1024
D = 768
HEADS = 6
KV_HEADS = 2
HEAD = 128
FF = 2304
LAYERS = 1
THETA = 10000
NAMES = ("wq", "wk", "wv", "wo", "w_gate", "w_up", "w_down")
SHAPES = {
    "wq": (LAYERS, D, HEADS * HEAD),
    "wk": (LAYERS, D, KV_HEADS * HEAD),
    "wv": (LAYERS, D, KV_HEADS * HEAD),
    "wo": (LAYERS, HEADS * HEAD, D),
    "w_gate": (LAYERS, D, FF),
    "w_up": (LAYERS, D, FF),
    "w_down": (LAYERS, FF, D),
}


def bump(key, n, height):
    away = (jnp.arange(n, dtype=jnp.int32) - jax.random.randint(key, (), 0, n, jnp.int32)) % n
    return jnp.where(away < n // 8, height, 1.0)


def together(key, own, strength):
    shared = jax.random.normal(key, own.shape[1:], jnp.float32)
    return (own + strength * shared) * lax.rsqrt(1 + strength * strength)


def setup_inputs(seed: int = 0, part: int = 0) -> dict:
    kx, kdy, ka, kb, kz, kf, kh, kl, *keys = jax.random.split(jax.random.key(seed), 8 + 3 * len(NAMES))
    kx, kdy, ka, kb = (jax.random.fold_in(k, part) for k in (kx, kdy, ka, kb))
    kw, km, kv = (keys[i::3] for i in range(3))
    shape = (SEQUENCES, TOKENS, D)
    much_x, much_dy = jax.random.uniform(kz, (2,), jnp.float32, 0.0, 1.0)
    loud = 2.0 ** jax.random.uniform(jax.random.fold_in(kz, 1), (), jnp.float32, -1.0, 2.0)
    layers = 2.0 ** jax.random.uniform(kl, (LAYERS, 1, 1), jnp.float32, -1.0, 1.0)
    times = {"wq": 1.0, "wk": 1.0, "wv": 2.0, "wo": layers, "w_gate": 1.0, "w_up": bump(kh, FF, 4.0), "w_down": layers}
    x = together(ka, jax.random.normal(kx, shape, jnp.float32), much_x) * bump(kf, D, 4.0)
    dy = together(kb, jax.random.normal(kdy, shape, jnp.float32), much_dy)
    drawn = {"x": x.astype(jnp.bfloat16), "dy": (loud * dy * (SEQUENCES * TOKENS) ** -0.5).astype(jnp.bfloat16)}
    for key, name in zip(kw, NAMES, strict=True):
        drawn[name] = (jax.random.normal(key, SHAPES[name], jnp.float32) * SHAPES[name][1] ** -0.5 * times[name]).astype(jnp.bfloat16)
    for key, name in zip(km, NAMES, strict=True):
        drawn[f"m_{name}"] = 0.1 * jax.random.normal(key, SHAPES[name], jnp.float32)
    for key, name in zip(kv, NAMES, strict=True):
        drawn[f"v_{name}"] = jax.random.uniform(key, SHAPES[name], jnp.float32, 0.02, 0.06)
    return drawn


def matmul(a, w):
    return jnp.dot(a, w, preferred_element_type=jnp.float32).astype(jnp.bfloat16)


def normed(h):
    wide = h.astype(jnp.float32)
    scale = lax.rsqrt(jnp.mean(wide**2, -1, keepdims=True) + 1e-6)
    return (wide * scale).astype(jnp.bfloat16)


def turned(t, theta):
    half = t.shape[-1] // 2
    angle = jnp.arange(t.shape[0], dtype=jnp.float32)[:, None] * theta ** (-jnp.arange(half, dtype=jnp.float32) / half)
    cos, sin = jnp.cos(angle)[:, None], jnp.sin(angle)[:, None]
    a, b = t[..., :half].astype(jnp.float32), t[..., half:].astype(jnp.float32)
    return jnp.concatenate([a * cos - b * sin, b * cos + a * sin], -1).astype(jnp.bfloat16)


def seen_by(q, k, v):
    tokens, kv = q.shape[0], k.shape[1]
    q = q.reshape(tokens, kv, -1, q.shape[-1])
    scores = jnp.einsum("tgsd,ugd->gstu", q.astype(jnp.float32), k.astype(jnp.float32)) * q.shape[-1] ** -0.5
    place = jnp.arange(tokens)
    weights = jax.nn.softmax(jnp.where(place[:, None] >= place, scores, -jnp.inf), -1).astype(jnp.bfloat16)
    return jnp.einsum("gstu,ugd->tgsd", weights.astype(jnp.float32), v.astype(jnp.float32)).astype(jnp.bfloat16).reshape(tokens, -1)


def layer(h, w):
    a = normed(h)
    q, k = (turned(matmul(a, w[name]).reshape(h.shape[0], -1, HEAD), THETA) for name in ("wq", "wk"))
    h = h + matmul(seen_by(q, k, matmul(a, w["wv"]).reshape(h.shape[0], -1, HEAD)), w["wo"])
    b = normed(h)
    gate = jnp.dot(b, w["w_gate"], preferred_element_type=jnp.float32)
    up = jnp.dot(b, w["w_up"], preferred_element_type=jnp.float32)
    return h + matmul((jax.nn.silu(gate) * up).astype(jnp.bfloat16), w["w_down"])


def adamw(w, m, v, g):
    m = 0.9 * m + 0.1 * g
    v = 0.95 * v + 0.05 * g * g
    step = m * lax.rsqrt(v + 1e-8) + 0.1 * w
    return (w - 0.02 * step).astype(jnp.bfloat16), m, v


def clipped(gradients, sum_of_squares, count):
    factor = jnp.minimum(1.0, 0.5 * lax.rsqrt(sum_of_squares / count + 1e-30))
    return [g * factor for g in gradients]


def stack(weights, h):
    return lax.scan(lambda h, w: (layer(h, w), None), h, weights)[0]


def reference(x, dy, wq, wk, wv, wo, w_gate, w_up, w_down, m_wq, m_wk, m_wv, m_wo, m_w_gate, m_w_up, m_w_down, v_wq, v_wk, v_wv, v_wo, v_w_gate, v_w_up, v_w_down):
    weights = dict(zip(NAMES, (wq, wk, wv, wo, w_gate, w_up, w_down), strict=True))

    def take(so_far, sequence):
        h, by_y = sequence
        _, back = jax.vjp(stack, weights, h)
        by_weights, by_h = back(by_y)
        return jax.tree.map(lambda total, term: total + term.astype(jnp.float32), so_far, by_weights), by_h

    none_yet = {name: jnp.zeros(w.shape, jnp.float32) for name, w in weights.items()}
    by_weights, by_x = lax.scan(take, none_yet, (x, dy))
    gradients = [by_weights[name].astype(jnp.bfloat16).astype(jnp.float32) for name in NAMES]
    gradients = clipped(gradients, sum(jnp.sum(g * g) for g in gradients), sum(g.size for g in gradients))
    first = (m_wq, m_wk, m_wv, m_wo, m_w_gate, m_w_up, m_w_down)
    second = (v_wq, v_wk, v_wv, v_wo, v_w_gate, v_w_up, v_w_down)
    new = [adamw(weights[name].astype(jnp.float32), m, v, g) for name, m, v, g in zip(NAMES, first, second, gradients, strict=True)]
    return tuple(one[which] for which in range(3) for one in new)
```

```python
import functools

import jax
import jax.numpy as jnp
import numpy as np
from jax import lax
from jax.experimental import pallas as pl
from jax.experimental.pallas import tpu as pltpu
from jax.sharding import PartitionSpec as P

MESH = pl.DeviceIdType.MESH
BF, F32 = jnp.bfloat16, jnp.float32
TOKENS, D, FF, HEAD = 1024, 768, 2304, 128
B = 256
BLOCKS = TOKENS // B
WIDE = 3 * B
T = 256
TILES = FF // T
HALF = D // 2
SCALE = HEAD**-0.5
LOG2E = 1.4426950408889634
E = SCALE * LOG2E
NEG = -1e30

COL, ROW = HALF // 8, T // 16
TILE = 6 * COL
WO = TILES * TILE
GROUPS = (WO + 6 * COL, 3200)
USED = GROUPS[0] + 5 * COL, GROUPS[1] + 5 * COL
UNIT = 128
ALL = 27 * UNIT


def span(i, n=B):
    return slice(i * n, (i + 1) * n)


def loop(n, body):
    lax.fori_loop(0, n, lambda i, _: (body(i), 0)[1], 0)


def places():
    me = lax.axis_index("dp")
    core, z, y, x = lax.rem(me, 2), lax.rem(lax.div(me, 2), 8), lax.rem(lax.div(me, 16), 4), lax.div(me, 64)

    def at(x, y, z, core):
        return ((x * 4 + y) * 8 + z) * 2 + core

    def four(i):
        return (lax.rem(lax.div(i + 1, 2), 2), i + 1 - 2 * lax.rem(i, 2)), (lax.div(i, 2), 3 - i)

    table = {"c": (core, [at(x, y, z, 1 - core)])}
    for name, (bit, p), (other, q) in zip("uv", four(x), four(y)):
        table["x" + name], table["y" + name] = (bit, [at(p, y, z, core)]), (other, [at(x, q, z, core)])
    table["X"] = x, [at(lax.rem(x + d, 4), y, z, core) for d in range(1, 4)]
    table["Y"] = y, [at(x, lax.rem(y + d, 4), z, core) for d in range(1, 4)]
    here = x * 4 + y
    table["P"] = here, [at(lax.div(lax.rem(here + d, 16), 4), lax.rem(here + d, 4), z, core) for d in range(1, 16)]
    table["Z"] = z, [at(x, y, lax.rem(z + d, 8), core) for d in range(1, 8)]
    for name, w in (("z", z), ("w", lax.rem(z + 7, 8))):
        odd = lax.rem(w, 2)
        table[name + "p"] = odd, [at(x, y, lax.rem(z + 9 - 2 * odd, 8), core)]
        table[name + "q"] = lax.div(w, 2), [at(x, y, lax.rem(z + 2 * d, 8), core) for d in range(1, 4)]
    return table, [p for name in "cPZ" for p in table[name][1]]


FLOWS = {"Aa": "xu xv Y Z", "Ab": "xv xu Y Z", "Ba": "yu yv X Z", "Bb": "yv yu X Z", "Ca": "zp zq X Y", "Cb": "wp wq Y X"}
FLOWS.update({"Ad": "X Y Z", "Bd": "Y X Z", "Pd": "P Z", "Zd": "Z P", "Cc": "zp zq P", "Cd": "wp wq P"})
FLOWS = {name: text.split() for name, text in FLOWS.items()}
GROUP = {"X": 4, "Y": 4, "Z": 8, "P": 16, "zq": 4, "wq": 4}

THETA = 10000
ORDER = "BdBbBaAaCaBaAdBbCaCbBaCbAdBaAdAdBd"
UNITS = [int(n) for n in "22221222211111212"]
SPLITS = (1, 2)
PACE = (1.5, 0.9, 1.5, 1.8, 1.4, 1.6, 3.6, 15.2)
RATE = (0.0032, 0.044, 0.0003, 0.0014)
EARLY = (1.4, 3.8, 4.6, 6.4, 6.8)
LATE = (1.2, 2.6, 3.4, 4.8, 5.3)
MOVE = 0.03
PATIENCE = 0.3

CHAINS, AFTER = [], []
for flow, units in zip([ORDER[i : i + 2] for i in range(0, len(ORDER), 2)], UNITS):
    CHAINS.append((flow, sum(n for _, _, n in CHAINS), units * UNIT))
    end = sum(n for _, _, n in CHAINS)
    ends = [((j, 2), (j + 1) * TILE) for j in range(TILES)] + [("o", USED[0] - 5 * COL), ((0, "d"), GROUPS[1]), ((1, "d"), ALL)]
    AFTER.append(next(place for place, n in ends if n >= end))


def last(c):
    return 2 * len(FLOWS[CHAINS[c][0]]) + 2


def sizes(c):
    flow, _, n = CHAINS[c]
    out = [n]
    for name in FLOWS[flow]:
        out.append(out[-1] // GROUP.get(name, 2))
    return out


def cost(c, what):
    names, size = FLOWS[CHAINS[c][0]], sizes(c)
    stages = len(names)
    k = what if what <= stages else last(c) - 1 - what
    work = MOVE
    if 0 < what <= stages + 1:
        work += (size[what - 1] - size[what] if what <= stages else size[stages]) * (what + 1) * RATE[2]
    if k == 0:
        return ["c"], size[0] * RATE[0], 0, work
    name = names[k - 1]
    kind = GROUP.get(name, 2)
    links = {"X": "xu xv", "Y": "yu yv", "P": "xu xv yu yv"}.get(name, name if kind == 2 else "zp wp").split()
    wire = size[k] * RATE[1] * (kind if name in "Z zq wq" else kind // 2)
    return links, wire, kind.bit_length() - 1, work


def plan():
    places = [((j, part), PACE[part]) for j in range(TILES) for part in range(3)] + [(("u", 1), PACE[3]), (("u", 3), PACE[3]), ("o", PACE[4])]
    for g in range(2):
        places += [((g, "b", r), PACE[5]) for r in SPLITS] + [((g, "d"), PACE[6])]
    due, done, free, moves, clock = {}, {}, {}, {}, PACE[-1]

    def move(c, what, delays):
        done[c] = what
        if what >= last(c):
            return MOVE
        links, wire, kind, work = cost(c, what)
        began = max([clock + work] + [free.get(link, 0.0) for link in links])
        free.update({link: began + wire for link in links})
        due[c] = began + wire + delays[kind]
        return work

    for place, time in places:
        clock += time
        for c, after in enumerate(AFTER):
            if after == place:
                due[c], done[c] = clock, -1
        moves[place] = []
        for t, c in sorted((t, c) for c, t in due.items() if t <= clock + PATIENCE and done[c] < last(c)):
            clock = max(clock, t)
            moves[place].append((c, done[c] + 1))
            clock += move(c, done[c] + 1, EARLY)
    moves["end"], squared = [], set()
    while len(squared) < len(CHAINS):
        t, c = min([(t, c) for c, t in due.items() if done[c] < last(c)] or [(clock + 9, -1)])
        ended = [c for c in due if done[c] == last(c) and c not in squared]
        if t > clock and ended:
            squared.add(ended[0])
            moves["end"].append((ended[0], last(ended[0]) + 1))
            clock += CHAINS[ended[0]][2] * RATE[3]
        else:
            clock = max(clock, t)
            moves["end"].append((c, done[c] + 1))
            clock += move(c, done[c] + 1, LATE)
    return moves, clock


class Sum:
    def __init__(self, g, mate, come, acc, sems):
        self.g, self.mate, self.come, self.acc = g, mate, come, acc
        self.down, self.up, self.free = sems
        self.table, self.near = places()
        self.core = self.table["c"][0]
        self.mine = []
        for c, (flow, _, _) in enumerate(CHAINS):
            mine = [0]
            for name, n in zip(FLOWS[flow], sizes(c)[1:]):
                mine.append(mine[-1] + self.table[name][0] * n)
            self.mine.append(mine)

    def greet(self):
        for p in self.near:
            pl.semaphore_signal(pltpu.get_barrier_semaphore(), inc=1, device_id={"dp": p}, device_id_type=MESH)

    def meet(self):
        pl.semaphore_wait(pltpu.get_barrier_semaphore(), len(self.near))

    def send(self, src, dst, sems, c, k, to):
        where = dict(send_sem=sems.at[0, c, k], recv_sem=sems.at[1, c, k], device_id={"dp": to}, device_id_type=MESH)
        pltpu.make_async_remote_copy(src_ref=src, dst_ref=dst, **where).start()

    def wait(self, sems, way, c, k):
        size = sizes(c)
        part = self.come.at[pl.ds(0, size[k - 1] - size[k] if k else size[0])]
        pltpu.make_async_copy(part, part, sems.at[way, c, k]).wait()

    def slot(self, c, k, d):
        size = sizes(c)
        return CHAINS[c][1] + size[0] - size[k - 1] + (d - 1) * size[k]

    def terms(self, c, k, at):
        _, base, _ = CHAINS[c]
        size, out = sizes(c), [(self.g.at[self.core], base + at), (self.mate, base + at)]
        for l in range(1, k):
            out += [(self.come, self.slot(c, l, d) + at - self.mine[c][l]) for d in range(1, size[l - 1] // size[l])]
        return out

    def add(self, terms, n, store):
        some = max(u for u in range(1, 33) if n % u == 0)

        def body(i):
            wide = [ref[pl.ds(start + i * some, some)].astype(F32) for ref, start in terms]
            store(i * some, some, functools.reduce(lambda a, b: a + b, wide))

        loop(n // some, body)

    def op(self, c, what):
        flow, base, n = CHAINS[c]
        names, size, mine = FLOWS[flow], sizes(c), self.mine[c]
        stages = len(names)
        mate = self.table["c"][1][0]
        if 0 < what <= stages + 1:
            self.wait(self.down, 1, c, what - 1)
        if what > last(c):
            return self.squares(c)
        if what > stages + 1:
            self.wait(self.up, 1, c, last(c) - what)
        if what == 0:
            self.send(self.g.at[1 - self.core, pl.ds(base, n)], self.mate.at[pl.ds(base, n)], self.down, c, 0, mate)
        elif what <= stages:
            if what == 1:
                self.wait(self.down, 0, c, 0)
                pl.semaphore_signal(self.free.at[c], inc=1, device_id={"dp": mate}, device_id_type=MESH)
            number, peers = self.table[names[what - 1]]
            for d, p in enumerate(peers, 1):
                at = mine[what - 1] + lax.rem(number + d, len(peers) + 1) * size[what]
                terms = self.terms(c, what, at)
                ref, start = terms[-1]

                def store(i, some, wide):
                    ref[pl.ds(start + i, some)] = wide.astype(BF)

                self.add(terms, size[what], store)
                self.send(ref.at[pl.ds(start, size[what])], self.come.at[pl.ds(self.slot(c, what, d), size[what])], self.down, c, what, p)
        elif what == stages + 1:

            def store(i, some, wide):
                self.g[self.core, pl.ds(base + mine[stages] + i, some)] = wide.astype(BF)

            self.add(self.terms(c, stages + 1, mine[stages]), size[stages], store)
        if stages < what < last(c):
            k = last(c) - 1 - what
            if k == 0:
                pl.semaphore_wait(self.free.at[c], 1)
            here = self.g.at[self.core, pl.ds(base + mine[k], size[k])]
            for p in self.table[names[k - 1] if k else "c"][1]:
                self.send(here, here, self.up, c, k, p)

    def squares(self, c):
        _, base, n = CHAINS[c]
        for half in range(2):

            def body(i):
                wide = self.g[half, pl.ds(base + i * 64, 64)].astype(F32).reshape(8, 8, 8, HEAD)
                self.acc[...] += jnp.sum(wide * wide, axis=0)

            loop(n // 64, body)

    def drain(self):
        for c, (flow, _, _) in enumerate(CHAINS):
            for k in range(len(FLOWS[flow]) + 1):
                self.wait(self.up, 0, c, k)
                if k > 0:
                    self.wait(self.down, 0, c, k)


def dot(a, b, ca=1, cb=0):
    return lax.dot_general(a, b, (((ca,), (cb,)), ((), ())), preferred_element_type=F32)


def blocks(body):
    loop(BLOCKS, lambda i: body(pl.ds(pl.multiple_of(i * B, B), B)))


def lanes(first, n=1):
    return pl.ds(pl.multiple_of(first * HEAD, HEAD), n * HEAD)


def turns():
    half = HEAD // 2
    step = THETA ** (-np.arange(half) / half)
    angles = [np.arange(32)[:, None] * n * np.concatenate([-step, step]) for n in (32, 1)]
    return np.stack([f(a) for a in angles for f in (np.cos, np.sin)]).astype(np.float32)


def tables(turn, cos_s, sin_s):
    fine_cos, fine_sin = turn[2], turn[3]

    def body(i):
        cos, sin = turn[0, pl.ds(i, 1)], turn[1, pl.ds(i, 1)]
        at = pl.ds(pl.multiple_of(i * 32, 32), 32)
        cos_s[at] = cos * fine_cos - sin * fine_sin
        sin_s[at] = sin * fine_cos + cos * fine_sin

    loop(32, body)


def normed(h):
    wide = h.astype(F32)
    scale = lax.rsqrt(jnp.mean(wide * wide, -1, keepdims=True) + 1e-6)
    return wide * scale, scale


def qkv(x_s, w_s, cos_s, sin_s, at_s, q_s, k_s, v_s, vt_s):
    def rows(at):
        a = normed(x_s[at])[0].astype(BF)
        at_s[:, at] = a.T
        cos, sin = cos_s[at], sin_s[at]
        for n in range(5):
            pair = dot(a, w_s[:, span(n, 2 * HEAD)]).astype(BF)
            for m in range(2):
                one = pair[:, span(m, HEAD)]
                if n < 4:
                    wide = one.astype(F32)
                    one = (wide * cos + pltpu.roll(wide, HEAD // 2, 1) * sin).astype(BF)
                if n < 3:
                    q_s[at, span(2 * n + m, HEAD)] = one
                elif n < 4:
                    k_s[m, at] = one
                else:
                    v_s[m, at] = one
                    vt_s[m, :HEAD, at] = one.T

    blocks(rows)
    vt_s[:, HEAD:] = jnp.ones((2, 8, TOKENS), BF)


def three(ref, g, at):
    return jnp.concatenate([ref[at, lanes(3 * g + n)] for n in range(3)], axis=0)


def later():
    return lax.rem(lax.broadcasted_iota(jnp.int32, (B, WIDE), 1), B) < lax.broadcasted_iota(jnp.int32, (B, WIDE), 0)


def attend(q_s, k_s, vt_s, s_s, o_s, ot_s, lse_s):
    def group(g):
        for r in range(BLOCKS):
            at = span(r)
            q, top, mix = three(q_s, g, at), None, None
            for b in range(r + 1):
                here = span(b)
                s = dot(k_s[g, here], q, 1, 1)
                if b == r:
                    s = jnp.where(later(), NEG, s)
                s_s[here] = s
                most = s.max(axis=0, keepdims=True)
                top = most if b == 0 else jnp.maximum(top, most)
            for b in range(r + 1):
                here = span(b)
                p = jnp.exp2((s_s[here] - top) * E).astype(BF)
                part = dot(vt_s[g, :, here], p)
                mix = part if b == 0 else mix + part
            total = mix[HEAD : HEAD + 1]
            out = (mix[:HEAD] * (1 / total)).astype(BF)
            lse = top * E + jnp.log2(total)
            for n in range(3):
                one = out[:, span(n)]
                ot_s[lanes(3 * g + n), at] = one
                o_s[at, lanes(3 * g + n)] = one.T
                lse_s[3 * g + n, :, at] = lse[:, span(n)]

    loop(2, group)


def project(x_s, o_s, wo_s, h_s, b_s, bt_s):
    def rows(at):
        h = (x_s[at].astype(F32) + dot(o_s[at], wo_s[...]).astype(BF).astype(F32)).astype(BF)
        h_s[at] = h
        b = normed(h)[0].astype(BF)
        b_s[at] = b
        bt_s[:, at] = b.T

    blocks(rows)


def hidden(w, wd, b_s, dy_s, dgu_s, act_s):
    for i in range(BLOCKS):
        at = span(i)
        both = dot(b_s[at], w[...])
        gate, up = both[:, :T], both[:, T:]
        by_act = dot(dy_s[at], wd[...], 1, 1).astype(BF).astype(F32)
        sig = 0.5 * jnp.tanh(0.5 * gate) + 0.5
        silu = gate * sig
        act_s[at] = (silu * up).astype(BF)
        dgu_s[at, T:] = (by_act * silu).astype(BF)
        dgu_s[at, :T] = (by_act * up * (sig + silu * (1 - sig))).astype(BF)


def put(g, half, base, dw):
    n, high = dw.shape[1] // HEAD, dw.shape[0] // 8
    for c in range(n):
        g[half, pl.ds(base + c * high, high)] = dw[:, span(c, HEAD)].astype(BF).reshape(high, 8, HEAD)


def hidden_back(w, base, dy_s, bt_s, dgu_s, act_s, db_s, g, between):
    for i in range(BLOCKS):
        at = span(i)
        db_s[at] += dot(dgu_s[at], w[...], 1, 1)
    between()
    for half in range(2):
        put(g, half, base, dot(bt_s[span(half, HALF)], dgu_s[...]))
    down = dot(act_s[...], dy_s[...], 0, 0)
    for half in range(2):
        put(g, half, base + 4 * COL, down[span(half, 8 * ROW)])


def unproject(h_s, dy_s, db_s, o_s, wo_s, dh_s, do_s, delta_s, between):
    def rows(at):
        unit, scale = normed(h_s[at])
        db = db_s[at].astype(BF).astype(F32)
        by_norm = (scale * (db - unit * jnp.mean(db * unit, -1, keepdims=True))).astype(BF).astype(F32)
        dh = (dy_s[at].astype(F32) + by_norm).astype(BF)
        dh_s[at] = dh
        do = dot(dh, wo_s[...], 1, 1).astype(BF)
        do_s[at] = do
        both = do.astype(F32) * o_s[at].astype(F32)
        for n in range(6):
            delta_s[n, :, at] = jnp.sum(both[:, span(n, HEAD)].T, axis=0, keepdims=True)

    for i in range(BLOCKS):
        rows(span(i))
        if i % 2:
            between(i)


def turned_back(wide, cos, sin):
    return wide * cos + pltpu.roll(wide * sin, HEAD // 2, 1)


def attend_back(i, q_s, k_s, v_s, do_s, lse_s, delta_s, cos_s, sin_s, dk_s, dv_s, kt_s, dqkv_s, between):
    for b in range(BLOCKS):
        kt_s[:, span(b)] = k_s[i, span(b)].T
    for r in range(BLOCKS):
        at = span(r)
        q, do, dqt = three(q_s, i, at), three(do_s, i, at), None
        lse, delta = (jnp.concatenate([ref[3 * i + n, :, at] for n in range(3)], axis=1) for ref in (lse_s, delta_s))
        for b in range(r + 1):
            here = span(b)
            p = jnp.exp2(dot(k_s[i, here], q, 1, 1) * E - lse)
            if b == r:
                p = jnp.where(later(), 0.0, p)
            ds = (p * (dot(v_s[i, here], do, 1, 1) - delta)).astype(BF)
            dv, dk = dot(p.astype(BF), do), dot(ds, q)
            if b == r:
                dv_s[here], dk_s[here] = dv, dk
            else:
                dv_s[here] += dv
                dk_s[here] += dk
            part = dot(kt_s[:, here], ds)
            dqt = part if b == 0 else dqt + part
        for n in range(3):
            dq = (dqt[:, span(n)] * SCALE).T.astype(BF).astype(F32)
            dqkv_s[at, span(n, HEAD)] = turned_back(dq, cos_s[at], sin_s[at]).astype(BF)
        if r in SPLITS:
            between(r)
    for r in range(BLOCKS):
        at = span(r)
        dk = (dk_s[at] * SCALE).astype(BF).astype(F32)
        dqkv_s[at, 3 * HEAD : 4 * HEAD] = turned_back(dk, cos_s[at], sin_s[at]).astype(BF)
        dqkv_s[at, 4 * HEAD :] = dv_s[at].astype(BF)


def train(x, dy, turn, wq, wk, wv, wo, wg, wu, wd, g, squares, x_s, dy_s, mate, come, w_s, wo_s, wgu_s, wd_s, cos_s, sin_s, at_s, q_s, k_s, v_s, vt_s, o_s, ot_s,
          lse_s, h_s, b_s, bt_s, dgu_s, act_s, db_s, delta_s, dk_s, dv_s, kt_s, dqkv_s, acc, down, up, free, sem, wsem):
    cm = Sum(g, mate, come, acc, (down, up, free))
    cm.greet()
    moves, _ = plan()

    def make(place):
        for c, what in moves[place]:
            cm.op(c, what)

    def make_if(test, place):
        if moves[place]:
            pl.when(test)(lambda: make(place))

    def tile(j, slot):
        units = pl.ds(pl.multiple_of(j * T, T), T)
        parts = [(wg.at[:, units], wgu_s.at[slot, :, pl.ds(0, T)]), (wu.at[:, units], wgu_s.at[slot, :, pl.ds(T, T)]), (wd.at[units], wd_s.at[slot])]
        return [pltpu.make_async_copy(src, dst, sem.at[slot, k]) for k, (src, dst) in enumerate(parts)]

    first = [(x, x_s), (wq, w_s.at[:, pl.ds(0, D)]), (wk, w_s.at[:, pl.ds(D, T)]), (wv, w_s.at[:, pl.ds(D + T, T)]), (wo, wo_s), (dy, dy_s)]
    first = [pltpu.make_async_copy(src, dst, wsem.at[k]) for k, (src, dst) in enumerate(first)]
    for copy in first + tile(0, 0):
        copy.start()
    for a, b in zip(USED, (GROUPS[1], ALL)):
        g[:, a:b] = jnp.zeros((2, b - a, 8, HEAD), BF)
    acc[...] = jnp.zeros_like(acc)
    tables(turn, cos_s, sin_s)
    for copy in first[:4]:
        copy.wait()
    qkv(x_s, w_s, cos_s, sin_s, at_s, q_s, k_s, v_s, vt_s)
    attend(q_s, k_s, vt_s, db_s, o_s, ot_s, lse_s)
    for copy in first[4:]:
        copy.wait()
    project(x_s, o_s, wo_s, h_s, b_s, bt_s)
    db_s[...] = jnp.zeros_like(db_s)
    cm.meet()

    def tiles(j):
        def between(part):
            for i in range(TILES):
                make_if(j == i, (i, part))

        slot = lax.rem(j, 2)
        for copy in tile(j, slot):
            copy.wait()

        @pl.when(j + 1 < TILES)
        def _():
            for copy in tile(j + 1, 1 - slot):
                copy.start()

        hidden(wgu_s.at[slot], wd_s.at[slot], b_s, dy_s, dgu_s, act_s)
        between(0)
        hidden_back(wgu_s.at[slot], j * TILE, dy_s, bt_s, dgu_s, act_s, db_s, g, lambda: between(1))
        between(2)

    loop(TILES, tiles)
    do_s, dh_s = b_s, x_s
    unproject(h_s, dy_s, db_s, o_s, wo_s, dh_s, do_s, delta_s, lambda i: make(("u", i)))
    for half in range(2):
        put(g, half, WO, dot(ot_s[span(half, HALF)], dh_s[...]))
    make("o")

    def group(i):
        def between(r):
            for n in range(2):
                make_if(i == n, (n, "b", r))

        attend_back(i, q_s, k_s, v_s, do_s, lse_s, delta_s, cos_s, sin_s, dk_s, dv_s, kt_s, dqkv_s, between)
        for half in range(2):
            put(g, half, GROUPS[0] + i * (GROUPS[1] - GROUPS[0]), dot(at_s[span(half, HALF)], dqkv_s[...]))
        for n in range(2):
            make_if(i == n, (n, "d"))

    loop(2, group)
    make("end")
    squares[...] = jnp.sum(acc[...], axis=0)
    cm.drain()


def gradients(x, dy, weights):
    vmem, anywhere, dma = pl.BlockSpec(memory_space=pltpu.VMEM), pl.BlockSpec(memory_space=pl.ANY), pltpu.SemaphoreType.DMA
    low = [(TOKENS, D), (TOKENS, D), (ALL, 8, HEAD), (ALL, 8, HEAD), (D, D + 2 * T), (D, D), (2, D, 2 * T), (2, T, D)]
    key = (2, TOKENS, HEAD)
    low2 = [(D, TOKENS), (TOKENS, D), key, key, (2, HEAD + 8, TOKENS), (TOKENS, D), (D, TOKENS)]
    low3 = [(TOKENS, D), (TOKENS, D), (D, TOKENS), (TOKENS, 2 * T), (TOKENS, T)]
    wide = pltpu.VMEM((TOKENS, D), F32)
    head, row = pltpu.VMEM((TOKENS, HEAD), F32), pltpu.VMEM((6, 1, TOKENS), F32)
    bf = lambda shapes: [pltpu.VMEM(s, BF) for s in shapes]
    scratch = bf(low) + [head, head] + bf(low2) + [row] + bf(low3) + [wide, row, head, head]
    scratch += bf([(HEAD, TOKENS), (TOKENS, 5 * HEAD)]) + [pltpu.VMEM((8, 8, HEAD), F32)]
    count = len(CHAINS)
    scratch += [dma((2, count, 5)), dma((2, count, 5)), pltpu.SemaphoreType.REGULAR((count,)), dma((2, 3)), dma((6,))]
    return pl.pallas_call(
        train,
        out_shape=[pltpu.VMEM((2, ALL, 8, HEAD), BF), pltpu.VMEM((8, HEAD), F32)],
        in_specs=[anywhere, anywhere, vmem] + [anywhere] * 7,
        out_specs=[vmem] * 2,
        scratch_shapes=scratch,
        compiler_params=pltpu.CompilerParams(collective_id=0, has_side_effects=True, vmem_limit_bytes=49 * 2**20),
        name="train",
    )(x, dy, jnp.asarray(turns()), *weights)


DEPTH, AHEAD = 36, 18
COUNT = 2 * D * D + 2 * D * T + 3 * D * FF
KINDS = "4", "5", "6", "0", "3", "12"
FIRST = np.cumsum([0] + [18] * 3 + [6] * 3).tolist()
TASKS = FIRST[-1]


def spot(kind, t):
    pairs = range(6)
    if kind < 2:
        third, row = lax.div(t, 6), lax.rem(t, 6)
        at = third * 3 * TILE + 2 * COL * kind + lax.rem(row, 3) * 16
        return row * 128, third * D, lax.div(row, 3), [at + n // 2 * TILE + n % 2 * COL for n in pairs]
    if kind == 2:
        at = lax.div(t, 2) * TILE + 4 * COL
        return t * 128, 0, lax.rem(t, 2), [at + n * ROW for n in pairs]
    step = GROUPS[1] - GROUPS[0]
    start, offsets = {
        3: (GROUPS[0], [n // 3 * step + n % 3 * COL for n in pairs]),
        4: (WO, [n * COL for n in pairs]),
        5: (GROUPS[0] + 3 * COL, [n % 2 * step + n // 2 % 2 * COL for n in pairs]),
    }[kind]
    return t * 128, 0, lax.div(t, 3), [start + lax.rem(t, 3) * 16 + n for n in offsets]


def adamw(squares, gs, *refs):
    old, new = ([refs[span(i + k, 7)] for i in range(3)] for k in (0, 3))
    *bufs, isem, osem = refs[42:]

    def copies(i, kind, out):
        names = [int(n) for n in KINDS[kind]]
        row, col, _, _ = spot(kind, i - FIRST[kind])
        slot, cs = lax.rem(i, DEPTH), []
        for k, buf in enumerate(bufs):
            for x, n in enumerate(names):
                rows, wide = pl.ds(pl.multiple_of(row, 128), 128), D if len(names) == 1 else T
                cols = pl.ds(pl.multiple_of(col, 128), wide) if kind < 2 else pl.ds(0, wide)
                part = buf.at[slot, :, pl.ds(x * T, wide)]
                if out:
                    cs.append(pltpu.make_async_copy(part, new[k][n].at[0, rows, cols], osem.at[slot, k]))
                else:
                    cs.append(pltpu.make_async_copy(old[k][n].at[0, rows, cols], part, isem.at[slot, k]))
        return cs

    def of(i, kind):
        return (i >= FIRST[kind]) & (i < FIRST[kind + 1])

    def go(i, out):
        for kind in range(len(KINDS)):

            @pl.when(of(i, kind))
            def _():
                for copy in copies(i, kind, out):
                    copy.start()

    def finish(i, out):
        for test, wide in ((i < FIRST[-2], D), (i >= FIRST[-2], 2 * T)):

            @pl.when(test)
            def _():
                for k, buf in enumerate(bufs):
                    part = buf.at[lax.rem(i, DEPTH), :, pl.ds(0, wide)]
                    pltpu.make_async_copy(part, part, (osem if out else isem).at[lax.rem(i, DEPTH), k]).wait()

    for i in range(AHEAD):
        go(jnp.int32(i), False)
    factor = jnp.minimum(1.0, 0.5 * lax.rsqrt(jnp.sum(squares[...], keepdims=True) / COUNT + 1e-30))

    def task(i):
        @pl.when(i + AHEAD < TASKS)
        def _():
            pl.when(i + AHEAD >= DEPTH)(lambda: finish(i + AHEAD - DEPTH, True))
            go(i + AHEAD, False)

        finish(i, False)
        where = [jnp.int32(0)] * 7
        for kind in range(len(KINDS)):
            _, _, half, ats = spot(kind, i - FIRST[kind])
            where = [jnp.where(of(i, kind), a, b) for a, b in zip([half, *ats], where)]
        wb, mb, vb = (buf.at[lax.rem(i, DEPTH)] for buf in bufs)
        for c in range(6):
            cols = span(c, HEAD)
            x = gs[where[0], pl.ds(where[c + 1], 16)].astype(F32).reshape(128, HEAD) * factor
            m = 0.9 * mb[:, cols] + 0.1 * x
            v = 0.95 * vb[:, cols] + 0.05 * x * x
            w = wb[:, cols].astype(F32)
            mb[:, cols] = m
            vb[:, cols] = v
            wb[:, cols] = (w - 0.02 * (m * lax.rsqrt(v + 1e-8) + 0.1 * w)).astype(BF)
        go(i, True)

    loop(TASKS, task)
    loop(DEPTH, lambda i: finish(TASKS - DEPTH + i, True))


held = pltpu.with_memory_space_constraint


def step(squares, g, arrays):
    anywhere, dma = pl.BlockSpec(memory_space=pltpu.HBM), pltpu.SemaphoreType.DMA
    return pl.pallas_call(
        adamw,
        out_shape=[jax.ShapeDtypeStruct(a.shape, a.dtype) for a in arrays],
        in_specs=[pl.BlockSpec(memory_space=pltpu.VMEM)] * 2 + [anywhere] * 21,
        out_specs=[anywhere] * 21,
        scratch_shapes=[*[pltpu.VMEM((DEPTH, 128, D), t) for t in (BF, F32, F32)], dma((DEPTH, 3)), dma((DEPTH, 3))],
        compiler_params=pltpu.CompilerParams(vmem_limit_bytes=49 * 2**20),
        name="adamw",
    )(held(squares, pltpu.VMEM), held(g, pltpu.VMEM), *[held(a, pltpu.HBM) for a in arrays])


def solution(mesh):
    def run(x, dy, *arrays):
        wq, wk, wv, wo, wg, wu, wd = (w[0] for w in arrays[:7])
        g, squares = gradients(x[0], dy[0], (wq, wk, wv, wo, wg, wu, wd))
        return tuple(step(squares, g, arrays))

    states, all_of = P(("rep", "dp")), P()
    return jax.shard_map(
        run,
        mesh=mesh,
        in_specs=(states, states) + (all_of,) * 21,
        out_specs=(P("rep"),) * 21,
        check_vma=False,
    )
```

```python
import functools

import jax
import jax.numpy as jnp
import numpy as np
from jax import lax
from jax.experimental import pallas as pl
from jax.experimental.pallas import tpu as pltpu
from jax.sharding import PartitionSpec as P

MESH = pl.DeviceIdType.MESH
BF, F32 = jnp.bfloat16, jnp.float32
TOKENS, D, FF, HEAD = 1024, 768, 2304, 128
B = 256
BLOCKS = TOKENS // B
WIDE = 3 * B
T = 256
TILES = FF // T
HALF = D // 2
SCALE = HEAD**-0.5
LOG2E = 1.4426950408889634
E = SCALE * LOG2E
NEG = -1e30

COL, ROW = HALF // 8, T // 16
TILE = 6 * COL
WO = TILES * TILE
GROUPS = (WO + 6 * COL, 3200)
USED = GROUPS[0] + 5 * COL, GROUPS[1] + 5 * COL
UNIT = 128
ALL = 27 * UNIT


def span(i, n=B):
    return slice(i * n, (i + 1) * n)


def loop(n, body):
    lax.fori_loop(0, n, lambda i, _: (body(i), 0)[1], 0)


def places():
    me = lax.axis_index("dp")
    core, z, y, x = lax.rem(me, 2), lax.rem(lax.div(me, 2), 8), lax.rem(lax.div(me, 16), 4), lax.div(me, 64)

    def at(x, y, z, core):
        return ((x * 4 + y) * 8 + z) * 2 + core

    def four(i):
        return (lax.rem(lax.div(i + 1, 2), 2), i + 1 - 2 * lax.rem(i, 2)), (lax.div(i, 2), 3 - i)

    table = {"c": (core, [at(x, y, z, 1 - core)])}
    for name, (bit, p), (other, q) in zip("uv", four(x), four(y)):
        table["x" + name], table["y" + name] = (bit, [at(p, y, z, core)]), (other, [at(x, q, z, core)])
    table["X"] = x, [at(lax.rem(x + d, 4), y, z, core) for d in range(1, 4)]
    table["Y"] = y, [at(x, lax.rem(y + d, 4), z, core) for d in range(1, 4)]
    table["Z"] = z, [at(x, y, lax.rem(z + d, 8), core) for d in range(1, 8)]
    for name, w in (("z", z), ("w", lax.rem(z + 7, 8))):
        odd = lax.rem(w, 2)
        table[name + "p"] = odd, [at(x, y, lax.rem(z + 9 - 2 * odd, 8), core)]
        table[name + "q"] = lax.div(w, 2), [at(x, y, lax.rem(z + 2 * d, 8), core) for d in range(1, 4)]
    return table, [p for name in "cXYZ" for p in table[name][1]]


FLOWS = {"Aa": "xu xv Y Z", "Ab": "xv xu Y Z", "Ba": "yu yv X Z", "Bb": "yv yu X Z", "Ca": "zp zq X Y", "Cb": "wp wq Y X"}
FLOWS.update({"Ad": "X Y Z", "Bd": "Y X Z"})
FLOWS = {name: text.split() for name, text in FLOWS.items()}
GROUP = {"X": 4, "Y": 4, "Z": 8, "zq": 4, "wq": 4}

THETA = 10000
ORDER = "CbBdBdBdBbAdBaBdAdCbAdCaBaAdAdBdAdAd"
UNITS = [int(n) for n in "212121222211111212"]
SPLITS = (1, 2)
PACE = (1.5, 0.9, 1.5, 1.8, 1.4, 1.6, 3.6, 15.2)
RATE = (0.0032, 0.044, 0.0003, 0.0014)
EARLY = (1.2, 3.0, 3.8, 5.4)
LATE = (1.2, 2.6, 3.4, 4.8)
MOVE = 0.03
PATIENCE = 0.3

CHAINS, AFTER = [], []
for flow, units in zip([ORDER[i : i + 2] for i in range(0, len(ORDER), 2)], UNITS):
    CHAINS.append((flow, sum(n for _, _, n in CHAINS), units * UNIT))
    end = sum(n for _, _, n in CHAINS)
    ends = [((j, 2), (j + 1) * TILE) for j in range(TILES)] + [("o", USED[0] - 5 * COL), ((0, "d"), GROUPS[1]), ((1, "d"), ALL)]
    AFTER.append(next(place for place, n in ends if n >= end))


def last(c):
    return 2 * len(FLOWS[CHAINS[c][0]]) + 2


def sizes(c):
    flow, _, n = CHAINS[c]
    out = [n]
    for name in FLOWS[flow]:
        out.append(out[-1] // GROUP.get(name, 2))
    return out


def cost(c, what):
    names, size = FLOWS[CHAINS[c][0]], sizes(c)
    stages = len(names)
    k = what if what <= stages else last(c) - 1 - what
    work = MOVE
    if 0 < what <= stages + 1:
        work += (size[what - 1] - size[what] if what <= stages else size[stages]) * (what + 1) * RATE[2]
    if k == 0:
        return ["c"], size[0] * RATE[0], 0, work
    name = names[k - 1]
    kind = GROUP.get(name, 2)
    links = {"X": "xu xv", "Y": "yu yv"}.get(name, name if kind == 2 else "zp wp").split()
    wire = size[k] * RATE[1] * (kind if name in "Z zq wq" else kind // 2)
    return links, wire, kind.bit_length() - 1, work


def plan():
    places = [((j, part), PACE[part]) for j in range(TILES) for part in range(3)] + [(("u", 1), PACE[3]), (("u", 3), PACE[3]), ("o", PACE[4])]
    for g in range(2):
        places += [((g, "b", r), PACE[5]) for r in SPLITS] + [((g, "d"), PACE[6])]
    due, done, free, moves, clock = {}, {}, {}, {}, PACE[-1]

    def move(c, what, delays):
        done[c] = what
        if what >= last(c):
            return MOVE
        links, wire, kind, work = cost(c, what)
        began = max([clock + work] + [free.get(link, 0.0) for link in links])
        free.update({link: began + wire for link in links})
        due[c] = began + wire + delays[kind]
        return work

    for place, time in places:
        clock += time
        for c, after in enumerate(AFTER):
            if after == place:
                due[c], done[c] = clock, -1
        moves[place] = []
        for t, c in sorted((t, c) for c, t in due.items() if t <= clock + PATIENCE and done[c] < last(c)):
            clock = max(clock, t)
            moves[place].append((c, done[c] + 1))
            clock += move(c, done[c] + 1, EARLY)
    moves["end"], squared = [], set()
    while len(squared) < len(CHAINS):
        t, c = min([(t, c) for c, t in due.items() if done[c] < last(c)] or [(clock + 9, -1)])
        ended = [c for c in due if done[c] == last(c) and c not in squared]
        if t > clock and ended:
            squared.add(ended[0])
            moves["end"].append((ended[0], last(ended[0]) + 1))
            clock += CHAINS[ended[0]][2] * RATE[3]
        else:
            clock = max(clock, t)
            moves["end"].append((c, done[c] + 1))
            clock += move(c, done[c] + 1, LATE)
    return moves, clock


class Sum:
    def __init__(self, g, mate, come, acc, sems):
        self.g, self.mate, self.come, self.acc = g, mate, come, acc
        self.down, self.up, self.free = sems
        self.table, self.near = places()
        self.core = self.table["c"][0]
        self.mine = []
        for c, (flow, _, _) in enumerate(CHAINS):
            mine = [0]
            for name, n in zip(FLOWS[flow], sizes(c)[1:]):
                mine.append(mine[-1] + self.table[name][0] * n)
            self.mine.append(mine)

    def greet(self):
        for p in self.near:
            pl.semaphore_signal(pltpu.get_barrier_semaphore(), inc=1, device_id={"dp": p}, device_id_type=MESH)

    def meet(self):
        pl.semaphore_wait(pltpu.get_barrier_semaphore(), len(self.near))

    def send(self, src, dst, sems, c, k, to):
        where = dict(send_sem=sems.at[0, c, k], recv_sem=sems.at[1, c, k], device_id={"dp": to}, device_id_type=MESH)
        pltpu.make_async_remote_copy(src_ref=src, dst_ref=dst, **where).start()

    def wait(self, sems, way, c, k):
        size = sizes(c)
        part = self.come.at[pl.ds(0, size[k - 1] - size[k] if k else size[0])]
        pltpu.make_async_copy(part, part, sems.at[way, c, k]).wait()

    def slot(self, c, k, d):
        size = sizes(c)
        return CHAINS[c][1] + size[0] - size[k - 1] + (d - 1) * size[k]

    def terms(self, c, k, at):
        _, base, _ = CHAINS[c]
        size, out = sizes(c), [(self.g.at[self.core], base + at), (self.mate, base + at)]
        for l in range(1, k):
            out += [(self.come, self.slot(c, l, d) + at - self.mine[c][l]) for d in range(1, size[l - 1] // size[l])]
        return out

    def add(self, terms, n, store):
        some = max(u for u in range(1, 33) if n % u == 0)

        def body(i):
            wide = [ref[pl.ds(start + i * some, some)].astype(F32) for ref, start in terms]
            store(i * some, some, functools.reduce(lambda a, b: a + b, wide))

        loop(n // some, body)

    def op(self, c, what):
        flow, base, n = CHAINS[c]
        names, size, mine = FLOWS[flow], sizes(c), self.mine[c]
        stages = len(names)
        mate = self.table["c"][1][0]
        if 0 < what <= stages + 1:
            self.wait(self.down, 1, c, what - 1)
        if what > last(c):
            return self.squares(c)
        if what > stages + 1:
            self.wait(self.up, 1, c, last(c) - what)
        if what == 0:
            self.send(self.g.at[1 - self.core, pl.ds(base, n)], self.mate.at[pl.ds(base, n)], self.down, c, 0, mate)
        elif what <= stages:
            if what == 1:
                self.wait(self.down, 0, c, 0)
                pl.semaphore_signal(self.free.at[c], inc=1, device_id={"dp": mate}, device_id_type=MESH)
            number, peers = self.table[names[what - 1]]
            for d, p in enumerate(peers, 1):
                at = mine[what - 1] + lax.rem(number + d, len(peers) + 1) * size[what]
                terms = self.terms(c, what, at)
                ref, start = terms[-1]

                def store(i, some, wide):
                    ref[pl.ds(start + i, some)] = wide.astype(BF)

                self.add(terms, size[what], store)
                self.send(ref.at[pl.ds(start, size[what])], self.come.at[pl.ds(self.slot(c, what, d), size[what])], self.down, c, what, p)
        elif what == stages + 1:

            def store(i, some, wide):
                self.g[self.core, pl.ds(base + mine[stages] + i, some)] = wide.astype(BF)

            self.add(self.terms(c, stages + 1, mine[stages]), size[stages], store)
        if stages < what < last(c):
            k = last(c) - 1 - what
            if k == 0:
                pl.semaphore_wait(self.free.at[c], 1)
            here = self.g.at[self.core, pl.ds(base + mine[k], size[k])]
            for p in self.table[names[k - 1] if k else "c"][1]:
                self.send(here, here, self.up, c, k, p)

    def squares(self, c):
        _, base, n = CHAINS[c]
        for half in range(2):

            def body(i):
                wide = self.g[half, pl.ds(base + i * 64, 64)].astype(F32).reshape(-1, *self.acc.shape)
                self.acc[...] += jnp.sum(wide * wide, axis=0)

            loop(n // 64, body)

    def drain(self):
        for c, (flow, _, _) in enumerate(CHAINS):
            for k in range(len(FLOWS[flow]) + 1):
                self.wait(self.up, 0, c, k)
                if k > 0:
                    self.wait(self.down, 0, c, k)


def dot(a, b, ca=1, cb=0):
    return lax.dot_general(a, b, (((ca,), (cb,)), ((), ())), preferred_element_type=F32)


def dot_t(a, b):
    return dot(a, b, 1, 1)


def blocks(body):
    for i in range(BLOCKS):
        body(span(i))


def lanes(first, n=1):
    return pl.ds(pl.multiple_of(first * HEAD, HEAD), n * HEAD)


def turns():
    half = HEAD // 2
    step = THETA ** (-np.arange(half) / half)
    angles = [np.arange(32)[:, None] * n * np.concatenate([-step, step]) for n in (32, 1)]
    return np.stack([f(a) for a in angles for f in (np.cos, np.sin)]).astype(np.float32)


def tables(turn, cos_s, sin_s):
    fine_cos, fine_sin = turn[2], turn[3]

    def body(i):
        cos, sin = turn[0, pl.ds(i, 1)], turn[1, pl.ds(i, 1)]
        at = pl.ds(pl.multiple_of(i * 32, 32), 32)
        cos_s[at] = cos * fine_cos - sin * fine_sin
        sin_s[at] = sin * fine_cos + cos * fine_sin

    loop(32, body)


def normed(h):
    wide = h.astype(F32)
    scale = lax.rsqrt(jnp.mean(wide * wide, -1, keepdims=True) + 1e-6)
    return wide * scale, scale


def qkv(x_s, w_s, cos_s, sin_s, at_s, q_s, k_s, v_s, vt_s):
    def rows(at):
        a = normed(x_s[at])[0].astype(BF)
        at_s[:, at] = a.T
        cos, sin = cos_s[at], sin_s[at]
        for n in range(5):
            pair = dot(a, w_s[:, span(n, 2 * HEAD)]).astype(BF)
            for m in range(2):
                one = pair[:, span(m, HEAD)]
                if n < 4:
                    wide = one.astype(F32)
                    one = (wide * cos + pltpu.roll(wide, HEAD // 2, 1) * sin).astype(BF)
                if n < 3:
                    q_s[at, span(2 * n + m, HEAD)] = one
                elif n < 4:
                    k_s[m, at] = one
                else:
                    v_s[m, at] = one
                    vt_s[m, :HEAD, at] = one.T

    blocks(rows)
    vt_s[:, HEAD:] = jnp.ones((2, 8, TOKENS), BF)


def three(ref, g, at):
    return jnp.concatenate([ref[at, lanes(3 * g + n)] for n in range(3)], axis=0)


def later():
    return lax.rem(lax.broadcasted_iota(jnp.int32, (B, WIDE), 1), B) < lax.broadcasted_iota(jnp.int32, (B, WIDE), 0)


def attend(q_s, k_s, vt_s, s_s, o_s, ot_s, lse_s):
    def group(g):
        for r in range(BLOCKS):
            at = span(r)
            q, top, mix = three(q_s, g, at), None, None
            for b in range(r + 1):
                here = span(b)
                s = dot_t(k_s[g, here], q)
                if b == r:
                    s = jnp.where(later(), NEG, s)
                s_s[here] = s
                most = s.max(axis=0, keepdims=True)
                top = most if b == 0 else jnp.maximum(top, most)
            for b in range(r + 1):
                here = span(b)
                p = jnp.exp2((s_s[here] - top) * E).astype(BF)
                part = dot(vt_s[g, :, here], p)
                mix = part if b == 0 else mix + part
            total = mix[HEAD : HEAD + 1]
            out = (mix[:HEAD] * (1 / total)).astype(BF)
            lse = top * E + jnp.log2(total)
            for n in range(3):
                one = out[:, span(n)]
                ot_s[lanes(3 * g + n), at] = one
                o_s[at, lanes(3 * g + n)] = one.T
                lse_s[3 * g + n, :, at] = lse[:, span(n)]

    loop(2, group)


def project(x_s, o_s, wo_s, h_s, b_s, bt_s):
    def rows(at):
        h = (x_s[at].astype(F32) + dot(o_s[at], wo_s[...]).astype(BF).astype(F32)).astype(BF)
        h_s[at] = h
        b = normed(h)[0].astype(BF)
        b_s[at] = b
        bt_s[:, at] = b.T

    blocks(rows)


def hidden(w, wd, b_s, dy_s, dgu_s, act_s):
    for i in range(BLOCKS):
        at = span(i)
        both = dot(b_s[at], w[...])
        gate, up = both[:, :T], both[:, T:]
        by_act = dot_t(dy_s[at], wd[...]).astype(BF).astype(F32)
        sig = 0.5 * jnp.tanh(0.5 * gate) + 0.5
        silu = gate * sig
        act_s[at] = (silu * up).astype(BF)
        dgu_s[at, T:] = (by_act * silu).astype(BF)
        dgu_s[at, :T] = (by_act * up * (sig + silu * (1 - sig))).astype(BF)


def put(g, half, base, dw):
    n, high = dw.shape[1] // HEAD, dw.shape[0] // 8
    for c in range(n):
        g[half, pl.ds(base + c * high, high)] = dw[:, span(c, HEAD)].astype(BF).reshape(high, 8, HEAD)


def hidden_back(w, base, dy_s, bt_s, dgu_s, act_s, db_s, g, between):
    for i in range(BLOCKS):
        at = span(i)
        db_s[at] += dot_t(dgu_s[at], w[...])
    between()
    for half in range(2):
        put(g, half, base, dot(bt_s[span(half, HALF)], dgu_s[...]))
    down = dot(act_s[...], dy_s[...], 0, 0)
    for half in range(2):
        put(g, half, base + 4 * COL, down[span(half, 8 * ROW)])


def unproject(h_s, dy_s, db_s, o_s, wo_s, dh_s, do_s, delta_s, between):
    def rows(at):
        unit, scale = normed(h_s[at])
        db = db_s[at].astype(BF).astype(F32)
        by_norm = (scale * (db - unit * jnp.mean(db * unit, -1, keepdims=True))).astype(BF).astype(F32)
        dh = (dy_s[at].astype(F32) + by_norm).astype(BF)
        dh_s[at] = dh
        do = dot_t(dh, wo_s[...]).astype(BF)
        do_s[at] = do
        both = do.astype(F32) * o_s[at].astype(F32)
        for n in range(6):
            delta_s[n, :, at] = jnp.sum(both[:, span(n, HEAD)].T, axis=0, keepdims=True)

    for i in range(BLOCKS):
        rows(span(i))
        if i % 2:
            between(i)


def turned_back(wide, cos, sin):
    return wide * cos + pltpu.roll(wide * sin, HEAD // 2, 1)


def attend_back(i, q_s, k_s, v_s, do_s, lse_s, delta_s, cos_s, sin_s, dk_s, dv_s, kt_s, dqkv_s, between):
    for b in range(BLOCKS):
        kt_s[:, span(b)] = k_s[i, span(b)].T
    for r in range(BLOCKS):
        at = span(r)
        q, do, dqt = three(q_s, i, at), three(do_s, i, at), None
        lse, delta = (jnp.concatenate([ref[3 * i + n, :, at] for n in range(3)], axis=1) for ref in (lse_s, delta_s))
        for b in range(r + 1):
            here = span(b)
            p = jnp.exp2(dot_t(k_s[i, here], q) * E - lse)
            if b == r:
                p = jnp.where(later(), 0.0, p)
            ds = (p * (dot_t(v_s[i, here], do) - delta)).astype(BF)
            dv, dk = dot(p.astype(BF), do), dot(ds, q)
            if b == r:
                dv_s[here], dk_s[here] = dv, dk
            else:
                dv_s[here] += dv
                dk_s[here] += dk
            part = dot(kt_s[:, here], ds)
            dqt = part if b == 0 else dqt + part
        for n in range(3):
            dq = (dqt[:, span(n)] * SCALE).T.astype(BF).astype(F32)
            dqkv_s[at, span(n, HEAD)] = turned_back(dq, cos_s[at], sin_s[at]).astype(BF)
        if r in SPLITS:
            between(r)
    for r in range(BLOCKS):
        at = span(r)
        dk = (dk_s[at] * SCALE).astype(BF).astype(F32)
        dqkv_s[at, 3 * HEAD : 4 * HEAD] = turned_back(dk, cos_s[at], sin_s[at]).astype(BF)
        dqkv_s[at, 4 * HEAD :] = dv_s[at].astype(BF)


def train(x, dy, turn, wq, wk, wv, wo, wg, wu, wd, m, g, squares, x_s, dy_s, q_s, o_s, h_s, b_s, wo_s, db_s, mate, come, w_s, wgu_s, wd_s, cos_s, sin_s, at_s, k_s, v_s, vt_s, ot_s,
          lse_s, bt_s, dgu_s, act_s, delta_s, dk_s, dv_s, kt_s, dqkv_s, acc, down, up, free, sem, wsem):
    cm = Sum(g, mate, come, acc, (down, up, free))
    cm.greet()
    moves, _ = plan()

    def make(place):
        for c, what in moves[place]:
            cm.op(c, what)

    def make_if(test, place):
        if moves[place]:
            pl.when(test)(lambda: make(place))

    def tile(j, slot):
        units = pl.ds(pl.multiple_of(j * T, T), T)
        parts = [(wg.at[:, units], wgu_s.at[slot, :, pl.ds(0, T)]), (wu.at[:, units], wgu_s.at[slot, :, pl.ds(T, T)]), (wd.at[units], wd_s.at[slot])]
        return [pltpu.make_async_copy(src, dst, sem.at[slot, k]) for k, (src, dst) in enumerate(parts)]

    first = [(x, x_s), (wq, w_s.at[:, pl.ds(0, D)]), (wk, w_s.at[:, pl.ds(D, T)]), (wv, w_s.at[:, pl.ds(D + T, T)]), (wo, wo_s), (dy, dy_s)]
    first = [pltpu.make_async_copy(src, dst, wsem.at[k]) for k, (src, dst) in enumerate(first)]
    for copy in first + tile(0, 0):
        copy.start()
    for a, b in zip(USED, (GROUPS[1], ALL)):
        g[:, a:b] = jnp.zeros((2, b - a, 8, HEAD), BF)
    acc[...] = jnp.zeros_like(acc)
    tables(turn, cos_s, sin_s)
    for copy in first[:4]:
        copy.wait()
    qkv(x_s, w_s, cos_s, sin_s, at_s, q_s, k_s, v_s, vt_s)
    attend(q_s, k_s, vt_s, db_s, o_s, ot_s, lse_s)
    for copy in first[4:]:
        copy.wait()
    project(x_s, o_s, wo_s, h_s, b_s, bt_s)
    db_s[...] = jnp.zeros_like(db_s)
    cm.meet()

    def tiles(j):
        def between(part):
            for i in range(TILES):
                make_if(j == i, (i, part))

        slot = lax.rem(j, 2)
        for copy in tile(j, slot):
            copy.wait()

        @pl.when(j + 1 < TILES)
        def _():
            for copy in tile(j + 1, 1 - slot):
                copy.start()

        hidden(wgu_s.at[slot], wd_s.at[slot], b_s, dy_s, dgu_s, act_s)
        between(0)
        hidden_back(wgu_s.at[slot], j * TILE, dy_s, bt_s, dgu_s, act_s, db_s, g, lambda: between(1))
        between(2)

    loop(TILES, tiles)
    do_s, dh_s = b_s, x_s
    unproject(h_s, dy_s, db_s, o_s, wo_s, dh_s, do_s, delta_s, lambda i: make(("u", i)))
    for half in range(2):
        put(g, half, WO, dot(ot_s[span(half, HALF)], dh_s[...]))
    make("o")
    done = x_s, dy_s, q_s, o_s, h_s, b_s, wo_s

    def fetch(*numbers):
        for n in numbers:
            for i in range(SOON * n, min(SOON * (n + 1), EARLIER)):
                where = window(i // 18, jnp.int32(i % 18))
                to = pl.ds(i % SOON * HEAD, HEAD)
                pltpu.make_async_copy((wg, wu, wd)[i // 18].at[where], done[n].at[to], wsem.at[6]).start()
                if n == 0:
                    pltpu.make_async_copy(m.at[where], db_s.at[to], wsem.at[7]).start()

    fetch(0, 1, 3, 4, 6)

    def group(i):
        def between(r):
            for n in range(2):
                make_if(i == n, (n, "b", r))

        attend_back(i, q_s, k_s, v_s, do_s, lse_s, delta_s, cos_s, sin_s, dk_s, dv_s, kt_s, dqkv_s, between)
        for half in range(2):
            put(g, half, GROUPS[0] + i * (GROUPS[1] - GROUPS[0]), dot(at_s[span(half, HALF)], dqkv_s[...]))
        for n in range(2):
            make_if(i == n, (n, "d"))

    loop(2, group)

    fetch(2, 5)
    make("end")
    for part in done:
        pltpu.make_async_copy(part, part, wsem.at[6]).wait()
    pltpu.make_async_copy(db_s, db_s, wsem.at[7]).wait()
    squares[...] = jnp.sum(acc[...], axis=0)
    cm.drain()


def gradients(x, dy, weights, m):
    vmem, anywhere, dma = pl.BlockSpec(memory_space=pltpu.VMEM), pl.BlockSpec(memory_space=pl.ANY), pltpu.SemaphoreType.DMA
    low = [(ALL, 8, HEAD), (ALL, 8, HEAD), (D, D + 2 * T), (2, D, 2 * T), (2, T, D)]
    key = (2, TOKENS, HEAD)
    low2 = [(D, TOKENS), key, key, (2, HEAD + 8, TOKENS), (D, TOKENS)]
    low3 = [(D, TOKENS), (TOKENS, 2 * T), (TOKENS, T)]
    head, row = pltpu.VMEM((TOKENS, HEAD), F32), pltpu.VMEM((6, 1, TOKENS), F32)
    bf = lambda shapes: [pltpu.VMEM(s, BF) for s in shapes]
    scratch = bf(low) + [head, head] + bf(low2) + [row] + bf(low3) + [row, head, head]
    scratch += bf([(HEAD, TOKENS), (TOKENS, 5 * HEAD)]) + [pltpu.VMEM((8, 8, HEAD), F32)]
    count = len(CHAINS)
    scratch += [dma((2, count, 5)), dma((2, count, 5)), pltpu.SemaphoreType.REGULAR((count,)), dma((2, 3)), dma((8,))]
    return pl.pallas_call(
        train,
        out_shape=[pltpu.VMEM((2, ALL, 8, HEAD), BF), pltpu.VMEM((8, HEAD), F32), *bf([(TOKENS, D)] * 6 + [(D, D)]), pltpu.VMEM((TOKENS, D), F32)],
        in_specs=[anywhere, anywhere, vmem] + [anywhere] * 8,
        out_specs=[vmem] * 10,
        scratch_shapes=scratch,
        compiler_params=pltpu.CompilerParams(collective_id=0, has_side_effects=True, vmem_limit_bytes=VMEM),
        name="train",
    )(x, dy, jnp.asarray(turns()), *weights, m)


DEPTH, AHEAD = 32, 16
COUNT = 2 * D * D + 2 * D * T + 3 * D * FF
KINDS = "4", "5", "6", "0", "3", "12"
FIRST = np.cumsum([0] + [18] * 3 + [6] * 3).tolist()
TASKS = FIRST[-1]
EARLIER, SOON = FIRST[3], TOKENS // HEAD
VMEM = 35 * 2**20


def spot(kind, t):
    pairs = range(6)
    if kind < 2:
        third, row = lax.div(t, 6), lax.rem(t, 6)
        at = third * 3 * TILE + 2 * COL * kind + lax.rem(row, 3) * 16
        return row * HEAD, third * D, lax.div(row, 3), [at + n // 2 * TILE + n % 2 * COL for n in pairs]
    if kind == 2:
        at = lax.div(t, 2) * TILE + 4 * COL
        return t * HEAD, 0, lax.rem(t, 2), [at + n * ROW for n in pairs]
    step = GROUPS[1] - GROUPS[0]
    start, offsets = {
        3: (GROUPS[0], [n // 3 * step + n % 3 * COL for n in pairs]),
        4: (WO, [n * COL for n in pairs]),
        5: (GROUPS[0] + 3 * COL, [n % 2 * step + n // 2 % 2 * COL for n in pairs]),
    }[kind]
    return t * HEAD, 0, lax.div(t, 3), [start + lax.rem(t, 3) * 16 + n for n in offsets]


def window(kind, t):
    row, col, _, _ = spot(kind, t)
    return pl.ds(pl.multiple_of(row, HEAD), HEAD), pl.ds(pl.multiple_of(col, HEAD), D) if kind < 2 else pl.ds(0, D)


def adamw(squares, gs, *refs):
    soon, refs = refs[:8], refs[8:]
    old, new = ([refs[span(i + k, 7)] for i in range(3)] for k in (0, 3))
    *bufs, isem, osem = refs[42:]

    def copies(i, kind, out):
        names = [int(n) for n in KINDS[kind]]
        rows, cols = window(kind, i - FIRST[kind])
        slot, cs = lax.rem(i, DEPTH), []
        for k, buf in enumerate(bufs):
            for x, n in enumerate(names):
                wide = D if len(names) == 1 else T
                cols = cols if len(names) == 1 else pl.ds(0, wide)
                part = buf.at[slot, :, pl.ds(x * T, wide)]
                if out:
                    cs.append((k, pltpu.make_async_copy(part, new[k][n].at[0, rows, cols], osem.at[slot, k])))
                else:
                    cs.append((k, pltpu.make_async_copy(old[k][n].at[0, rows, cols], part, isem.at[slot, k])))
        return cs

    def there(i, k):
        return (i < EARLIER) if k == 0 else (i < SOON) if k == 1 else (i < 0)

    def of(i, kind):
        return (i >= FIRST[kind]) & (i < FIRST[kind + 1])

    def go(i, out):
        for kind in range(len(KINDS)):

            @pl.when(of(i, kind))
            def _():
                for k, copy in copies(i, kind, out):
                    pl.when(out | ~there(i, k))(copy.start)

    def finish(i, out):
        for test, wide in ((i < FIRST[-2], D), (i >= FIRST[-2], 2 * T)):

            @pl.when(test)
            def _():
                for k, buf in enumerate(bufs):
                    part = buf.at[lax.rem(i, DEPTH), :, pl.ds(0, wide)]
                    pl.when(out | ~there(i, k))(pltpu.make_async_copy(part, part, (osem if out else isem).at[lax.rem(i, DEPTH), k]).wait)

    for i in range(AHEAD):
        go(jnp.int32(i), False)
    factor = jnp.minimum(1.0, 0.5 * lax.rsqrt(jnp.sum(squares[...], keepdims=True) / COUNT + 1e-30))

    def task(i, group):
        @pl.when(i + AHEAD < TASKS)
        def _():
            pl.when(i + AHEAD >= DEPTH)(lambda: finish(i + AHEAD - DEPTH, True))
            go(i + AHEAD, False)

        finish(i, False)
        where = [jnp.int32(0)] * 7
        for kind in range(len(KINDS)):
            _, _, half, ats = spot(kind, i - FIRST[kind])
            where = [jnp.where(of(i, kind), a, b) for a, b in zip([half, *ats], where)]
        wb, mb, vb = (buf.at[lax.rem(i, DEPTH)] for buf in bufs)
        rows = pl.ds(pl.multiple_of(lax.rem(i, SOON) * HEAD, HEAD), HEAD)
        from_w, from_m = soon[group].at[rows] if group < 7 else wb, soon[7].at[rows] if group == 0 else mb
        for c in range(6):
            cols = span(c, HEAD)
            x = gs[where[0], pl.ds(where[c + 1], 16)].astype(F32).reshape(HEAD, HEAD) * factor
            m = 0.9 * from_m[:, cols] + 0.1 * x
            v = 0.95 * vb[:, cols] + 0.05 * x * x
            w = from_w[:, cols].astype(F32)
            mb[:, cols] = m
            vb[:, cols] = v
            wb[:, cols] = (w - 0.02 * (m * lax.rsqrt(v + 1e-8) + 0.1 * w)).astype(BF)
        go(i, True)

    starts = [*range(0, EARLIER, SOON), EARLIER, TASKS]
    for group, first in enumerate(starts[:-1]):
        loop(starts[group + 1] - first, lambda i: task(first + i, group))
    loop(DEPTH, lambda i: finish(TASKS - DEPTH + i, True))


held = pltpu.with_memory_space_constraint


def step(taken, arrays):
    anywhere, dma = pl.BlockSpec(memory_space=pltpu.HBM), pltpu.SemaphoreType.DMA
    return pl.pallas_call(
        adamw,
        out_shape=[jax.ShapeDtypeStruct(a.shape, a.dtype) for a in arrays],
        in_specs=[pl.BlockSpec(memory_space=pltpu.VMEM)] * 10 + [anywhere] * 21,
        out_specs=[anywhere] * 21,
        scratch_shapes=[*[pltpu.VMEM((DEPTH, HEAD, D), t) for t in (BF, F32, F32)], dma((DEPTH, 3)), dma((DEPTH, 3))],
        compiler_params=pltpu.CompilerParams(vmem_limit_bytes=VMEM),
        name="adamw",
    )(*[held(a, pltpu.VMEM) for a in taken], *[held(a, pltpu.HBM) for a in arrays])


def solution(mesh):
    def run(x, dy, *arrays):
        wq, wk, wv, wo, wg, wu, wd = (w[0] for w in arrays[:7])
        g, squares, *soon = gradients(x[0], dy[0], (wq, wk, wv, wo, wg, wu, wd), arrays[11][0])
        return tuple(step((squares, g, *soon), arrays))

    states, all_of = P(("rep", "dp")), P()
    return jax.shard_map(
        run,
        mesh=mesh,
        in_specs=(states, states) + (all_of,) * 21,
        out_specs=(P("rep"),) * 21,
        check_vma=False,
    )
```

```python
import functools

import jax
import jax.numpy as jnp
import numpy as np
from jax import lax
from jax.experimental import pallas as pl
from jax.experimental.pallas import tpu as pltpu
from jax.sharding import PartitionSpec as P

MESH = pl.DeviceIdType.MESH
BF, F32 = jnp.bfloat16, jnp.float32
TOKENS, D, FF, HEAD = 1024, 768, 2304, 128
B = 256
BLOCKS = TOKENS // B
WIDE = 3 * B
T = 256
TILES = FF // T
HALF = D // 2
SCALE = HEAD**-0.5
LOG2E = 1.4426950408889634
E = SCALE * LOG2E
NEG = -1e30

COL, ROW = HALF // 8, T // 16
TILE = 6 * COL
WO = TILES * TILE
GROUPS = (WO + 6 * COL, 3200)
USED = GROUPS[0] + 5 * COL, GROUPS[1] + 5 * COL
UNIT = 128
ALL = 27 * UNIT


def span(i, n=B):
    return slice(i * n, (i + 1) * n)


def loop(n, body):
    lax.fori_loop(0, n, lambda i, _: (body(i), 0)[1], 0)


def places():
    me = lax.axis_index("dp")
    core, z, y, x = lax.rem(me, 2), lax.rem(lax.div(me, 2), 8), lax.rem(lax.div(me, 16), 4), lax.div(me, 64)

    def at(x, y, z, core):
        return ((x * 4 + y) * 8 + z) * 2 + core

    def four(i):
        return (lax.rem(lax.div(i + 1, 2), 2), i + 1 - 2 * lax.rem(i, 2)), (lax.div(i, 2), 3 - i)

    table = {"c": (core, [at(x, y, z, 1 - core)])}
    for name, (bit, p), (other, q) in zip("uv", four(x), four(y)):
        table["x" + name], table["y" + name] = (bit, [at(p, y, z, core)]), (other, [at(x, q, z, core)])
    table["X"] = x, [at(lax.rem(x + d, 4), y, z, core) for d in range(1, 4)]
    table["Y"] = y, [at(x, lax.rem(y + d, 4), z, core) for d in range(1, 4)]
    table["Z"] = z, [at(x, y, lax.rem(z + d, 8), core) for d in range(1, 8)]
    for name, w in (("z", z), ("w", lax.rem(z + 7, 8))):
        odd = lax.rem(w, 2)
        table[name + "p"] = odd, [at(x, y, lax.rem(z + 9 - 2 * odd, 8), core)]
        table[name + "q"] = lax.div(w, 2), [at(x, y, lax.rem(z + 2 * d, 8), core) for d in range(1, 4)]
    return table, [p for name in "cXYZ" for p in table[name][1]]


FLOWS = {"Aa": "xu xv Y Z", "Ab": "xv xu Y Z", "Ba": "yu yv X Z", "Bb": "yv yu X Z", "Ca": "zp zq X Y", "Cb": "wp wq Y X"}
FLOWS.update({"Ad": "X Y Z", "Bd": "Y X Z"})
FLOWS = {name: text.split() for name, text in FLOWS.items()}
GROUP = {"X": 4, "Y": 4, "Z": 8, "zq": 4, "wq": 4}

THETA = 10000
ORDER = "BdAdCbAdCaBdAdCaAdCbBdAdCbBdBdAdAdBd"
UNITS = [int(n) for n in "211112222112112212"]
SPLITS = (1, 2)
PACE = (1.5, 0.0, 2.3, 1.8, 1.4, 1.6, 3.6, 14.4)
RATE = (0.0034, 0.04, 0.0003, 0.0014)
EARLY = (2.36, 3.66, 4.6, 5.81)
LATE = (2.49, 2.05, 2.13, 3.27)
MOVE = 0.03
PATIENCE = 0.15

CHAINS, AFTER = [], []
for flow, units in zip([ORDER[i : i + 2] for i in range(0, len(ORDER), 2)], UNITS):
    CHAINS.append((flow, sum(n for _, _, n in CHAINS), units * UNIT))
    end = sum(n for _, _, n in CHAINS)
    ends = [((j, 2), (j + 1) * TILE) for j in range(TILES)] + [("o", USED[0] - 5 * COL), ((0, "d"), GROUPS[1]), ((1, "d"), ALL)]
    AFTER.append(next(place for place, n in ends if n >= end))


def last(c):
    return 2 * len(FLOWS[CHAINS[c][0]]) + 2


def sizes(c):
    flow, _, n = CHAINS[c]
    out = [n]
    for name in FLOWS[flow]:
        out.append(out[-1] // GROUP.get(name, 2))
    return out


def cost(c, what):
    names, size = FLOWS[CHAINS[c][0]], sizes(c)
    stages = len(names)
    k = what if what <= stages else last(c) - 1 - what
    work = MOVE
    if 0 < what <= stages + 1:
        work += (size[what - 1] - size[what] if what <= stages else size[stages]) * (what + 1) * RATE[2]
    if k == 0:
        return ["c"], size[0] * RATE[0], 0, work
    name = names[k - 1]
    kind = GROUP.get(name, 2)
    links = {"X": "xu xv", "Y": "yu yv"}.get(name, name if kind == 2 else "zp wp").split()
    wire = size[k] * RATE[1] * (kind if name in "Z zq wq" else kind // 2)
    return links, wire, kind.bit_length() - 1, work


def plan():
    places = [((j, part), PACE[part]) for j in range(TILES) for part in (0, 2)] + [(("u", 1), PACE[3]), (("u", 3), PACE[3]), ("o", PACE[4])]
    for g in range(2):
        places += [((g, "b", r), PACE[5]) for r in SPLITS] + [((g, "d"), PACE[6])]
    due, done, free, moves, clock = {}, {}, {}, {}, PACE[-1]

    def move(c, what, delays):
        done[c] = what
        if what >= last(c):
            return MOVE
        links, wire, kind, work = cost(c, what)
        began = max([clock + work] + [free.get(link, 0.0) for link in links])
        free.update({link: began + wire for link in links})
        due[c] = began + wire + delays[kind]
        return work

    for place, time in places:
        clock += time
        for c, after in enumerate(AFTER):
            if after == place:
                due[c], done[c] = clock, -1
        moves[place] = []
        for t, c in sorted((t, c) for c, t in due.items() if t <= clock + PATIENCE and done[c] < last(c)):
            clock = max(clock, t)
            moves[place].append((c, done[c] + 1))
            clock += move(c, done[c] + 1, EARLY)
    moves["end"], squared = [], set()
    while len(squared) < len(CHAINS):
        t, c = min([(t, c) for c, t in due.items() if done[c] < last(c)] or [(clock + 9, -1)])
        ended = [c for c in due if done[c] == last(c) and c not in squared]
        if t > clock and ended:
            squared.add(ended[0])
            moves["end"].append((ended[0], last(ended[0]) + 1))
            clock += CHAINS[ended[0]][2] * RATE[3]
        else:
            clock = max(clock, t)
            moves["end"].append((c, done[c] + 1))
            clock += move(c, done[c] + 1, LATE)
    return moves, clock


class Sum:
    def __init__(self, g, mate, come, acc, sems):
        self.g, self.mate, self.come, self.acc = g, mate, come, acc
        self.down, self.up, self.free = sems
        self.table, self.near = places()
        self.core = self.table["c"][0]
        self.mine = []
        for c, (flow, _, _) in enumerate(CHAINS):
            mine = [0]
            for name, n in zip(FLOWS[flow], sizes(c)[1:]):
                mine.append(mine[-1] + self.table[name][0] * n)
            self.mine.append(mine)

    def greet(self):
        for p in self.near:
            pl.semaphore_signal(pltpu.get_barrier_semaphore(), inc=1, device_id={"dp": p}, device_id_type=MESH)

    def meet(self):
        pl.semaphore_wait(pltpu.get_barrier_semaphore(), len(self.near))

    def send(self, src, dst, sems, c, k, to):
        where = dict(send_sem=sems.at[0, c, k], recv_sem=sems.at[1, c, k], device_id={"dp": to}, device_id_type=MESH)
        pltpu.make_async_remote_copy(src_ref=src, dst_ref=dst, **where).start()

    def wait(self, sems, way, c, k):
        size = sizes(c)
        part = self.come.at[pl.ds(0, size[k - 1] - size[k] if k else size[0])]
        pltpu.make_async_copy(part, part, sems.at[way, c, k]).wait()

    def slot(self, c, k, d):
        size = sizes(c)
        return CHAINS[c][1] + size[0] - size[k - 1] + (d - 1) * size[k]

    def terms(self, c, k, at):
        _, base, _ = CHAINS[c]
        size, out = sizes(c), [(self.g.at[self.core], base + at), (self.mate, base + at)]
        for l in range(1, k):
            out += [(self.come, self.slot(c, l, d) + at - self.mine[c][l]) for d in range(1, size[l - 1] // size[l])]
        return out

    def add(self, terms, n, store):
        some = max(u for u in range(1, 33) if n % u == 0)

        def body(i):
            wide = [ref[pl.ds(start + i * some, some)].astype(F32) for ref, start in terms]
            store(i * some, some, functools.reduce(lambda a, b: a + b, wide))

        loop(n // some, body)

    def op(self, c, what):
        flow, base, n = CHAINS[c]
        names, size, mine = FLOWS[flow], sizes(c), self.mine[c]
        stages = len(names)
        mate = self.table["c"][1][0]
        if 0 < what <= stages + 1:
            self.wait(self.down, 1, c, what - 1)
        if what > last(c):
            return self.squares(c)
        if what > stages + 1:
            self.wait(self.up, 1, c, last(c) - what)
        if what == 0:
            self.send(self.g.at[1 - self.core, pl.ds(base, n)], self.mate.at[pl.ds(base, n)], self.down, c, 0, mate)
        elif what <= stages:
            if what == 1:
                self.wait(self.down, 0, c, 0)
                pl.semaphore_signal(self.free.at[c], inc=1, device_id={"dp": mate}, device_id_type=MESH)
            number, peers = self.table[names[what - 1]]
            for d, p in enumerate(peers, 1):
                at = mine[what - 1] + lax.rem(number + d, len(peers) + 1) * size[what]
                terms = self.terms(c, what, at)
                ref, start = terms[-1]

                def store(i, some, wide):
                    ref[pl.ds(start + i, some)] = wide.astype(BF)

                self.add(terms, size[what], store)
                self.send(ref.at[pl.ds(start, size[what])], self.come.at[pl.ds(self.slot(c, what, d), size[what])], self.down, c, what, p)
        elif what == stages + 1:

            def store(i, some, wide):
                self.g[self.core, pl.ds(base + mine[stages] + i, some)] = wide.astype(BF)

            self.add(self.terms(c, stages + 1, mine[stages]), size[stages], store)
        if stages < what < last(c):
            k = last(c) - 1 - what
            if k == 0:
                pl.semaphore_wait(self.free.at[c], 1)
            here = self.g.at[self.core, pl.ds(base + mine[k], size[k])]
            for p in self.table[names[k - 1] if k else "c"][1]:
                self.send(here, here, self.up, c, k, p)

    def squares(self, c):
        _, base, n = CHAINS[c]
        for half in range(2):

            def body(i):
                wide = self.g[half, pl.ds(base + i * 64, 64)].astype(F32).reshape(-1, *self.acc.shape)
                self.acc[...] += jnp.sum(wide * wide, axis=0)

            loop(n // 64, body)

    def drain(self):
        for c, (flow, _, _) in enumerate(CHAINS):
            for k in range(len(FLOWS[flow]) + 1):
                self.wait(self.up, 0, c, k)
                if k > 0:
                    self.wait(self.down, 0, c, k)


def dot(a, b, ca=1, cb=0):
    return lax.dot_general(a, b, (((ca,), (cb,)), ((), ())), preferred_element_type=F32)


def dot_t(a, b):
    return dot(a, b, 1, 1)


def blocks(body):
    for i in range(BLOCKS):
        body(span(i))


def lanes(first, n=1):
    return pl.ds(pl.multiple_of(first * HEAD, HEAD), n * HEAD)


def turns():
    half = HEAD // 2
    step = THETA ** (-np.arange(half) / half)
    angles = [np.arange(32)[:, None] * n * np.concatenate([-step, step]) for n in (32, 1)]
    return np.stack([f(a) for a in angles for f in (np.cos, np.sin)]).astype(np.float32)


def tables(turn, cos_s, sin_s):
    fine_cos, fine_sin = turn[2], turn[3]

    def body(i):
        cos, sin = turn[0, pl.ds(i, 1)], turn[1, pl.ds(i, 1)]
        at = pl.ds(pl.multiple_of(i * 32, 32), 32)
        cos_s[at] = cos * fine_cos - sin * fine_sin
        sin_s[at] = sin * fine_cos + cos * fine_sin

    loop(32, body)


def normed(h):
    wide = h.astype(F32)
    scale = lax.rsqrt(jnp.mean(wide * wide, -1, keepdims=True) + 1e-6)
    return wide * scale, scale


def qkv(x_s, w_s, cos_s, sin_s, at_s, q_s, k_s, v_s, vt_s):
    def rows(at):
        a = normed(x_s[at])[0].astype(BF)
        at_s[:, at] = a.T
        cos, sin = cos_s[at], sin_s[at]
        for n in range(5):
            pair = dot(a, w_s[:, span(n, 2 * HEAD)]).astype(BF)
            for m in range(2):
                one = pair[:, span(m, HEAD)]
                if n < 4:
                    wide = one.astype(F32)
                    one = (wide * cos + pltpu.roll(wide, HEAD // 2, 1) * sin).astype(BF)
                if n < 3:
                    q_s[at, span(2 * n + m, HEAD)] = one
                elif n < 4:
                    k_s[m, at] = one
                else:
                    v_s[m, at] = one
                    vt_s[m, :HEAD, at] = one.T

    blocks(rows)
    vt_s[:, HEAD:] = jnp.ones((2, 8, TOKENS), BF)


def three(ref, g, at):
    return jnp.concatenate([ref[at, lanes(3 * g + n)] for n in range(3)], axis=0)


def later():
    return lax.rem(lax.broadcasted_iota(jnp.int32, (B, WIDE), 1), B) < lax.broadcasted_iota(jnp.int32, (B, WIDE), 0)


def attend(q_s, k_s, vt_s, s_s, o_s, ot_s, lse_s):
    def group(g):
        for r in range(BLOCKS):
            at = span(r)
            q, top, mix = three(q_s, g, at), None, None
            for b in range(r + 1):
                here = span(b)
                s = dot_t(k_s[g, here], q)
                if b == r:
                    s = jnp.where(later(), NEG, s)
                s_s[here] = s
                most = s.max(axis=0, keepdims=True)
                top = most if b == 0 else jnp.maximum(top, most)
            for b in range(r + 1):
                here = span(b)
                p = jnp.exp2((s_s[here] - top) * E).astype(BF)
                part = dot(vt_s[g, :, here], p)
                mix = part if b == 0 else mix + part
            total = mix[HEAD : HEAD + 1]
            out = (mix[:HEAD] * (1 / total)).astype(BF)
            lse = top * E + jnp.log2(total)
            for n in range(3):
                one = out[:, span(n)]
                ot_s[lanes(3 * g + n), at] = one
                o_s[at, lanes(3 * g + n)] = one.T
                lse_s[3 * g + n, :, at] = lse[:, span(n)]

    loop(2, group)


def project(x_s, o_s, wo_s, h_s, b_s, bt_s):
    def rows(at):
        h = (x_s[at].astype(F32) + dot(o_s[at], wo_s[...]).astype(BF).astype(F32)).astype(BF)
        h_s[at] = h
        b = normed(h)[0].astype(BF)
        b_s[at] = b
        bt_s[:, at] = b.T

    blocks(rows)


def hidden(w, wd, b_s, dy_s, dgu_s, act_s):
    for i in range(BLOCKS):
        at = span(i)
        both = dot(b_s[at], w[...])
        gate, up = both[:, :T], both[:, T:]
        by_act = dot_t(dy_s[at], wd[...]).astype(BF).astype(F32)
        sig = 0.5 * jnp.tanh(0.5 * gate) + 0.5
        silu = gate * sig
        act_s[at] = (silu * up).astype(BF)
        dgu_s[at, T:] = (by_act * silu).astype(BF)
        dgu_s[at, :T] = (by_act * up * (sig + silu * (1 - sig))).astype(BF)


def put(g, half, base, dw):
    n, high = dw.shape[1] // HEAD, dw.shape[0] // 8
    for c in range(n):
        g[half, pl.ds(base + c * high, high)] = dw[:, span(c, HEAD)].astype(BF).reshape(high, 8, HEAD)


def hidden_back(w, base, dy_s, bt_s, dgu_s, act_s, db_s, g):
    for i in range(BLOCKS):
        at = span(i)
        db_s[at] += dot_t(dgu_s[at], w[...])
    for half in range(2):
        put(g, half, base, dot(bt_s[span(half, HALF)], dgu_s[...]))
    down = dot(act_s[...], dy_s[...], 0, 0)
    for half in range(2):
        put(g, half, base + 4 * COL, down[span(half, 8 * ROW)])


def unproject(h_s, dy_s, db_s, o_s, wo_s, dh_s, do_s, delta_s, between):
    def rows(at):
        unit, scale = normed(h_s[at])
        db = db_s[at].astype(BF).astype(F32)
        by_norm = (scale * (db - unit * jnp.mean(db * unit, -1, keepdims=True))).astype(BF).astype(F32)
        dh = (dy_s[at].astype(F32) + by_norm).astype(BF)
        dh_s[at] = dh
        do = dot_t(dh, wo_s[...]).astype(BF)
        do_s[at] = do
        both = do.astype(F32) * o_s[at].astype(F32)
        for n in range(6):
            delta_s[n, :, at] = jnp.sum(both[:, span(n, HEAD)].T, axis=0, keepdims=True)

    for i in range(BLOCKS):
        rows(span(i))
        if i % 2:
            between(i)


def turned_back(wide, cos, sin):
    return wide * cos + pltpu.roll(wide * sin, HEAD // 2, 1)


def attend_back(i, q_s, k_s, v_s, do_s, lse_s, delta_s, cos_s, sin_s, dk_s, dv_s, kt_s, dqkv_s, between):
    for b in range(BLOCKS):
        kt_s[:, span(b)] = k_s[i, span(b)].T
    for r in range(BLOCKS):
        at = span(r)
        q, do, dqt = three(q_s, i, at), three(do_s, i, at), None
        lse, delta = (jnp.concatenate([ref[3 * i + n, :, at] for n in range(3)], axis=1) for ref in (lse_s, delta_s))
        for b in range(r + 1):
            here = span(b)
            p = jnp.exp2(dot_t(k_s[i, here], q) * E - lse)
            if b == r:
                p = jnp.where(later(), 0.0, p)
            ds = (p * (dot_t(v_s[i, here], do) - delta)).astype(BF)
            dv, dk = dot(p.astype(BF), do), dot(ds, q)
            if b == r:
                dv_s[here], dk_s[here] = dv, dk
            else:
                dv_s[here] += dv
                dk_s[here] += dk
            part = dot(kt_s[:, here], ds)
            dqt = part if b == 0 else dqt + part
        for n in range(3):
            dq = (dqt[:, span(n)] * SCALE).T.astype(BF).astype(F32)
            dqkv_s[at, span(n, HEAD)] = turned_back(dq, cos_s[at], sin_s[at]).astype(BF)
        if r in SPLITS:
            between(r)
    for r in range(BLOCKS):
        at = span(r)
        dk = (dk_s[at] * SCALE).astype(BF).astype(F32)
        dqkv_s[at, 3 * HEAD : 4 * HEAD] = turned_back(dk, cos_s[at], sin_s[at]).astype(BF)
        dqkv_s[at, 4 * HEAD :] = dv_s[at].astype(BF)


def train(x, dy, turn, wq, wk, wv, wo, wg, wu, wd, m, v, g, squares, x_s, dy_s, q_s, o_s, h_s, b_s, wo_s, db_s, mate, come, w_s, wgu_s, wd_s, cos_s, sin_s, at_s, k_s, v_s, vt_s, ot_s,
          lse_s, bt_s, dgu_s, act_s, delta_s, dk_s, dv_s, kt_s, dqkv_s, acc, down, up, free, sem, wsem):
    cm = Sum(g, mate, come, acc, (down, up, free))
    cm.greet()
    moves, _ = plan()

    def make(place):
        for c, what in moves[place]:
            cm.op(c, what)

    def make_if(test, place):
        if moves[place]:
            pl.when(test)(lambda: make(place))

    def tile(j, slot):
        units = pl.ds(pl.multiple_of(j * T, T), T)
        parts = [(wg.at[:, units], wgu_s.at[slot, :, pl.ds(0, T)]), (wu.at[:, units], wgu_s.at[slot, :, pl.ds(T, T)]), (wd.at[units], wd_s.at[slot])]
        return [pltpu.make_async_copy(src, dst, sem.at[slot, k]) for k, (src, dst) in enumerate(parts)]

    first = [(x, x_s), (wq, w_s.at[:, pl.ds(0, D)]), (wk, w_s.at[:, pl.ds(D, T)]), (wv, w_s.at[:, pl.ds(D + T, T)]), (wo, wo_s), (dy, dy_s)]
    first = [pltpu.make_async_copy(src, dst, wsem.at[k]) for k, (src, dst) in enumerate(first)]
    for copy in first[:4]:
        copy.start()
    for a, b in zip(USED, (GROUPS[1], ALL)):
        g[:, a:b] = jnp.zeros((2, b - a, 8, HEAD), BF)
    acc[...] = jnp.zeros_like(acc)
    tables(turn, cos_s, sin_s)
    for copy in first[:4]:
        copy.wait()
    for copy in first[4:] + tile(0, 0):
        copy.start()
    qkv(x_s, w_s, cos_s, sin_s, at_s, q_s, k_s, v_s, vt_s)
    attend(q_s, k_s, vt_s, db_s, o_s, ot_s, lse_s)
    for copy in first[4:]:
        copy.wait()
    project(x_s, o_s, wo_s, h_s, b_s, bt_s)
    db_s[...] = jnp.zeros_like(db_s)
    cm.meet()

    def tiles(j):
        def between(part):
            for i in range(TILES):
                make_if(j == i, (i, part))

        slot = lax.rem(j, 2)
        for copy in tile(j, slot):
            copy.wait()

        @pl.when(j + 1 < TILES)
        def _():
            for copy in tile(j + 1, 1 - slot):
                copy.start()

        hidden(wgu_s.at[slot], wd_s.at[slot], b_s, dy_s, dgu_s, act_s)
        between(0)
        hidden_back(wgu_s.at[slot], j * TILE, dy_s, bt_s, dgu_s, act_s, db_s, g)
        between(2)

    loop(TILES, tiles)
    do_s, dh_s = b_s, x_s
    unproject(h_s, dy_s, db_s, o_s, wo_s, dh_s, do_s, delta_s, lambda i: make(("u", i)))
    for half in range(2):
        put(g, half, WO, dot(ot_s[span(half, HALF)], dh_s[...]))
    make("o")
    done = x_s, dy_s, q_s, o_s, h_s, b_s, wo_s

    def fetch(*numbers):
        for n in numbers:
            for i in range(SOON * n, min(SOON * (n + 1), EARLIER)):
                where = window(i // 18, jnp.int32(i % 18))
                to = pl.ds(i % SOON * HEAD, HEAD)
                pltpu.make_async_copy((wg, wu, wd)[i // 18].at[where], done[n].at[to], wsem.at[6]).start()
                if i < BOTH:
                    for k, ref in enumerate((m, v)):
                        pltpu.make_async_copy(ref.at[where], db_s.at[pl.ds((k * BOTH + i) * HEAD, HEAD)], wsem.at[7]).start()

    fetch(0, 1, 3, 4, 6)

    def group(i):
        def between(r):
            for n in range(2):
                make_if(i == n, (n, "b", r))

        attend_back(i, q_s, k_s, v_s, do_s, lse_s, delta_s, cos_s, sin_s, dk_s, dv_s, kt_s, dqkv_s, between)
        for half in range(2):
            put(g, half, GROUPS[0] + i * (GROUPS[1] - GROUPS[0]), dot(at_s[span(half, HALF)], dqkv_s[...]))
        for n in range(2):
            make_if(i == n, (n, "d"))

    loop(2, group)

    fetch(2, 5)
    make("end")
    for part in done:
        pltpu.make_async_copy(part, part, wsem.at[6]).wait()
    pltpu.make_async_copy(db_s, db_s, wsem.at[7]).wait()
    squares[...] = jnp.sum(acc[...], axis=0)
    cm.drain()


def gradients(x, dy, weights, m, v):
    vmem, anywhere, dma = pl.BlockSpec(memory_space=pltpu.VMEM), pl.BlockSpec(memory_space=pl.ANY), pltpu.SemaphoreType.DMA
    low = [(ALL, 8, HEAD), (ALL, 8, HEAD), (D, D + 2 * T), (2, D, 2 * T), (2, T, D)]
    key = (2, TOKENS, HEAD)
    low2 = [(D, TOKENS), key, key, (2, HEAD + 8, TOKENS), (D, TOKENS)]
    low3 = [(D, TOKENS), (TOKENS, 2 * T), (TOKENS, T)]
    head, row = pltpu.VMEM((TOKENS, HEAD), F32), pltpu.VMEM((6, 1, TOKENS), F32)
    bf = lambda shapes: [pltpu.VMEM(s, BF) for s in shapes]
    scratch = bf(low) + [head, head] + bf(low2) + [row] + bf(low3) + [row, head, head]
    scratch += bf([(HEAD, TOKENS), (TOKENS, 5 * HEAD)]) + [pltpu.VMEM((8, 8, HEAD), F32)]
    count = len(CHAINS)
    scratch += [dma((2, count, 5)), dma((2, count, 5)), pltpu.SemaphoreType.REGULAR((count,)), dma((2, 3)), dma((8,))]
    return pl.pallas_call(
        train,
        out_shape=[pltpu.VMEM((2, ALL, 8, HEAD), BF), pltpu.VMEM((8, HEAD), F32), *bf([(TOKENS, D)] * 6 + [(D, D)]), pltpu.VMEM((TOKENS, D), F32)],
        in_specs=[anywhere, anywhere, vmem] + [anywhere] * 9,
        out_specs=[vmem] * 10,
        scratch_shapes=scratch,
        compiler_params=pltpu.CompilerParams(collective_id=0, has_side_effects=True, vmem_limit_bytes=VMEM),
        name="train",
    )(x, dy, jnp.asarray(turns()), *weights, m, v)


DEPTH, AHEAD = 32, 16
COUNT = 2 * D * D + 2 * D * T + 3 * D * FF
KINDS = "4", "5", "6", "0", "3", "12"
FIRST = np.cumsum([0] + [18] * 3 + [6] * 3).tolist()
TASKS = FIRST[-1]
EARLIER, SOON = FIRST[3], TOKENS // HEAD
BOTH = SOON // 2
VMEM = 35 * 2**20


def spot(kind, t):
    pairs = range(6)
    if kind < 2:
        third, row = lax.div(t, 6), lax.rem(t, 6)
        at = third * 3 * TILE + 2 * COL * kind + lax.rem(row, 3) * 16
        return row * HEAD, third * D, lax.div(row, 3), [at + n // 2 * TILE + n % 2 * COL for n in pairs]
    if kind == 2:
        at = lax.div(t, 2) * TILE + 4 * COL
        return t * HEAD, 0, lax.rem(t, 2), [at + n * ROW for n in pairs]
    step = GROUPS[1] - GROUPS[0]
    start, offsets = {
        3: (GROUPS[0], [n // 3 * step + n % 3 * COL for n in pairs]),
        4: (WO, [n * COL for n in pairs]),
        5: (GROUPS[0] + 3 * COL, [n % 2 * step + n // 2 % 2 * COL for n in pairs]),
    }[kind]
    return t * HEAD, 0, lax.div(t, 3), [start + lax.rem(t, 3) * 16 + n for n in offsets]


def window(kind, t):
    row, col, _, _ = spot(kind, t)
    return pl.ds(pl.multiple_of(row, HEAD), HEAD), pl.ds(pl.multiple_of(col, HEAD), D) if kind < 2 else pl.ds(0, D)


def adamw(squares, gs, *refs):
    soon, refs = refs[:8], refs[8:]
    old, new = ([refs[span(i + k, 7)] for i in range(3)] for k in (0, 3))
    *bufs, isem, osem = refs[42:]

    def copies(i, kind, out):
        names = [int(n) for n in KINDS[kind]]
        rows, cols = window(kind, i - FIRST[kind])
        slot, cs = lax.rem(i, DEPTH), []
        for k, buf in enumerate(bufs):
            for x, n in enumerate(names):
                wide = D if len(names) == 1 else T
                cols = cols if len(names) == 1 else pl.ds(0, wide)
                part = buf.at[slot, :, pl.ds(x * T, wide)]
                if out:
                    cs.append((k, pltpu.make_async_copy(part, new[k][n].at[0, rows, cols], osem.at[slot, k])))
                else:
                    cs.append((k, pltpu.make_async_copy(old[k][n].at[0, rows, cols], part, isem.at[slot, k])))
        return cs

    def there(i, k):
        return i < (BOTH if k else EARLIER)

    def of(i, kind):
        return (i >= FIRST[kind]) & (i < FIRST[kind + 1])

    def go(i, out):
        for kind in range(len(KINDS)):

            @pl.when(of(i, kind))
            def _():
                for k, copy in copies(i, kind, out):
                    pl.when(out | ~there(i, k))(copy.start)

    def finish(i, out):
        for test, wide in ((i < FIRST[-2], D), (i >= FIRST[-2], 2 * T)):

            @pl.when(test)
            def _():
                for k, buf in enumerate(bufs):
                    part = buf.at[lax.rem(i, DEPTH), :, pl.ds(0, wide)]
                    pl.when(out | ~there(i, k))(pltpu.make_async_copy(part, part, (osem if out else isem).at[lax.rem(i, DEPTH), k]).wait)

    for i in range(AHEAD):
        go(jnp.int32(i), False)
    factor = jnp.minimum(1.0, 0.5 * lax.rsqrt(jnp.sum(squares[...], keepdims=True) / COUNT + 1e-30))

    def task(i, first):
        @pl.when(i + AHEAD < TASKS)
        def _():
            pl.when(i + AHEAD >= DEPTH)(lambda: finish(i + AHEAD - DEPTH, True))
            go(i + AHEAD, False)

        finish(i, False)
        where = [jnp.int32(0)] * 7
        for kind in range(len(KINDS)):
            _, _, half, ats = spot(kind, i - FIRST[kind])
            where = [jnp.where(of(i, kind), a, b) for a, b in zip([half, *ats], where)]
        wb, mb, vb = (buf.at[lax.rem(i, DEPTH)] for buf in bufs)
        at = pl.multiple_of(lax.rem(i, SOON) * HEAD, HEAD)
        from_w = soon[first // SOON].at[pl.ds(at, HEAD)] if first < EARLIER else wb
        from_m, from_v = (soon[7].at[pl.ds(at + k * BOTH * HEAD, HEAD)] if first < BOTH else buf for k, buf in enumerate((mb, vb)))
        for c in range(6):
            cols = span(c, HEAD)
            x = gs[where[0], pl.ds(where[c + 1], 16)].astype(F32).reshape(HEAD, HEAD) * factor
            m = 0.9 * from_m[:, cols] + 0.1 * x
            v = 0.95 * from_v[:, cols] + 0.05 * x * x
            w = from_w[:, cols].astype(F32)
            mb[:, cols] = m
            vb[:, cols] = v
            wb[:, cols] = (w - 0.02 * (m * lax.rsqrt(v + 1e-8) + 0.1 * w)).astype(BF)
        go(i, True)

    starts = [0, BOTH, *range(SOON, EARLIER, SOON), EARLIER, TASKS]
    for first, end in zip(starts, starts[1:]):
        loop(end - first, lambda i: task(first + i, first))
    loop(DEPTH, lambda i: finish(TASKS - DEPTH + i, True))


held = pltpu.with_memory_space_constraint


def step(taken, arrays):
    anywhere, dma = pl.BlockSpec(memory_space=pltpu.HBM), pltpu.SemaphoreType.DMA
    return pl.pallas_call(
        adamw,
        out_shape=[jax.ShapeDtypeStruct(a.shape, a.dtype) for a in arrays],
        in_specs=[pl.BlockSpec(memory_space=pltpu.VMEM)] * 10 + [anywhere] * 21,
        out_specs=[anywhere] * 21,
        scratch_shapes=[*[pltpu.VMEM((DEPTH, HEAD, D), t) for t in (BF, F32, F32)], dma((DEPTH, 3)), dma((DEPTH, 3))],
        compiler_params=pltpu.CompilerParams(vmem_limit_bytes=VMEM),
        name="adamw",
    )(*[held(a, pltpu.VMEM) for a in taken], *[held(a, pltpu.HBM) for a in arrays])


def solution(mesh):
    def run(x, dy, *arrays):
        wq, wk, wv, wo, wg, wu, wd = (w[0] for w in arrays[:7])
        g, squares, *soon = gradients(x[0], dy[0], (wq, wk, wv, wo, wg, wu, wd), arrays[11][0], arrays[18][0])
        return tuple(step((squares, g, *soon), arrays))

    states, all_of = P(("rep", "dp")), P()
    return jax.shard_map(
        run,
        mesh=mesh,
        in_specs=(states, states) + (all_of,) * 21,
        out_specs=(P("rep"),) * 21,
        check_vma=False,
    )
```
